128 devices in a mesh: ctx: 32 (over y, z, core), mp: 4 (over x).
Axes of the slice: x: 4, y: 4, z: 4, core: 2. Of those that a mesh axis runs over, the one named last changes fastest.
Arguments:
- queries: bfloat16 [65536, 2048], P('ctx', 'mp'), may hold values from -6 to 6
- key_vectors: bfloat16 [65536, 2048], P('ctx', 'mp'), may hold values from -6 to 6
- value_vectors: bfloat16 [65536, 2048], P('ctx', 'mp'), may hold values from -6 to 6
- level_index: int32 [65536], P('ctx'), may hold values from 0 to 15
- level_table: float32 [16, 16, 20], P(None, 'mp'), may hold values from 0.1 to 4
- out_weight: bfloat16 [2048, 2048], P('mp'), may hold values from -0.125 to 0.125
Outputs:
- layer_out: bfloat16 [65536, 2048], P(('ctx', 'mp'))
The draws below stay inside these ranges and needn't reach their ends.
All inputs are finite; a program needn't handle non-finite values.
Results may differ from the reference program's by a relative error of at most 0.015.
Values may be sent and summed in bfloat16 or wider, within the bound.
A program may use at most 128 MiB of HBM per device.

```python
import math
import jax
import jax.numpy as jnp
from jax import lax

D = 2048
H = 16
DH = 128
STRETCH = 256
PLANS = 16
LEVELS = 20
TOKENS = 65536
N_MP = 4


def with_ends(array, key, low, top_value):
    shape = array.shape
    spot = [jax.random.randint(jax.random.fold_in(key, axis), (), 0, shape[axis]) for axis in range(len(shape))]
    array = array.at[tuple(spot)].set(low)
    longest = shape.index(max(shape))
    spot[longest] = (spot[longest] + 1) % shape[longest]
    return array.at[tuple(spot)].set(top_value)


def steps_of(rng, dims, shards, smallest, top_value):
    factor_of = 1.0
    for axis_at, blocks in shards:
        heights = jax.random.uniform(jax.random.fold_in(jax.random.fold_in(rng, 6), axis_at), (blocks,), jnp.float32, smallest / len(shards), top_value / len(shards))
        factor_of = factor_of * jnp.repeat(jnp.exp(heights), dims[axis_at] // blocks).reshape((-1,) + (1,) * (len(dims) - 1 - axis_at))
    return factor_of


def bell_draw(own_key, dims, width, bound, cuts=(), kind=jnp.bfloat16):
    result = width * jax.random.normal(own_key, dims, jnp.float32)
    if cuts:
        result = result * steps_of(own_key, dims, cuts, -0.22, 0.18)
    return jnp.clip(result, -bound, bound).astype(kind)


def setup_inputs(seed: int = 0) -> dict:
    keys = jax.random.split(jax.random.key(seed), 7)
    queries = bell_draw(keys[0], (TOKENS, H * DH), 1.0, 6.0, ((0, 32), (1, 4)))
    key_vectors = bell_draw(keys[1], (TOKENS, H * DH), 1.0, 6.0, ((0, 32), (1, 4)))
    value_vectors = bell_draw(keys[2], (TOKENS, H * DH), 1.0, 6.0, ((0, 32), (1, 4)))
    level_index = with_ends(jax.random.randint(keys[3], (TOKENS,), 0, PLANS), jax.random.fold_in(keys[3], 1), 0, PLANS - 1).astype(jnp.int32)
    level_table = jnp.clip(jnp.exp(math.log(4.0) - 3.6888794 * jax.random.uniform(keys[4], (PLANS, H, LEVELS), jnp.float32) ** steps_of(keys[4], (PLANS, H, LEVELS), ((1, 4),), -0.2, 0.2)), 0.1, 4.0)
    out_weight = bell_draw(keys[5], (H * DH, D), (H * DH) ** -0.5, 0.125, ((0, 4),))
    return dict(queries=queries, key_vectors=key_vectors, value_vectors=value_vectors, level_index=level_index, level_table=level_table, out_weight=out_weight)


EPSILON = 1e-06

def fenwick_level(offsets, digits):
    counted = jnp.zeros(offsets.shape, jnp.int32)
    for bit_index in range(digits):
        counted = counted + (offsets >= 1 << bit_index).astype(jnp.int32)
    return counted

def head_output(inputs):
    head_queries, head_keys, head_values, head_weights = inputs
    stretch_count = TOKENS // STRETCH
    stretch_bits = STRETCH.bit_length() - 1
    global_bits = stretch_count.bit_length() - 1
    query_blocks = head_queries.reshape(stretch_count, STRETCH, DH)
    key_blocks = head_keys.reshape(stretch_count, STRETCH, DH)
    value_blocks = head_values.reshape(stretch_count, STRETCH, DH)
    weight_blocks = head_weights.reshape(stretch_count, STRETCH, LEVELS)
    scores = jnp.einsum('ntd,nsd->nts', query_blocks.astype(jnp.float32), key_blocks.astype(jnp.float32))
    positions = jnp.arange(STRETCH, dtype=jnp.int32)
    relative = jnp.bitwise_xor(positions[:, None], positions[None, :])
    levels = fenwick_level(relative, stretch_bits + 1)
    causal = positions[None, :] <= positions[:, None]
    picked = jnp.take_along_axis(weight_blocks, jnp.broadcast_to(levels[None], (stretch_count, STRETCH, STRETCH)).astype(jnp.int32), axis=2)
    weighted = jnp.where(causal[None], scores * picked, 0.0).astype(jnp.bfloat16)
    output = jnp.einsum('nts,nse->nte', weighted.astype(jnp.float32), value_blocks.astype(jnp.float32))
    states = jnp.einsum('nsd,nse->nde', key_blocks.astype(jnp.float32), value_blocks.astype(jnp.float32))
    for bit_index in range(global_bits):
        span_width = 1 << bit_index
        groups = stretch_count // (2 * span_width)
        lower_states = states.reshape(groups, 2, span_width, DH, DH)[:, 0].sum(axis=1)
        lower_states = lax.optimization_barrier(lower_states.astype(jnp.bfloat16)).astype(jnp.float32)
        upper_rows = query_blocks.reshape(groups, 2, span_width * STRETCH, DH)[:, 1].astype(jnp.float32)
        reached = jnp.einsum('gtd,gde->gte', upper_rows, lower_states, precision=lax.Precision.HIGHEST)
        level_scale = weight_blocks.reshape(groups, 2, span_width * STRETCH, LEVELS)[:, 1, :, stretch_bits + 1 + bit_index]
        contribution = reached * level_scale[..., None]
        padded = jnp.stack([jnp.zeros_like(contribution), contribution], axis=1).reshape(stretch_count, STRETCH, DH)
        output = output + padded
    output = output.reshape(TOKENS, DH)
    normed = output * lax.rsqrt(lax.optimization_barrier(jnp.mean(output * output, axis=-1, keepdims=True)) + EPSILON)
    return normed.astype(jnp.bfloat16)

def reference(queries, key_vectors, value_vectors, level_index, level_table, out_weight):
    token_weights = level_table[level_index]
    head_queries = queries.reshape(TOKENS, H, DH).transpose(1, 0, 2)
    head_keys = key_vectors.reshape(TOKENS, H, DH).transpose(1, 0, 2)
    head_values = value_vectors.reshape(TOKENS, H, DH).transpose(1, 0, 2)
    head_weights = token_weights.transpose(1, 0, 2)
    head_rows = lax.map(head_output, (head_queries, head_keys, head_values, head_weights))
    mixed = head_rows.transpose(1, 0, 2).reshape(TOKENS, H * DH)
    group_cols = H * DH // N_MP
    summed = jnp.zeros((TOKENS, D), jnp.float32)
    for group_id in range(N_MP):
        share_out = jnp.dot(mixed[:, group_id * group_cols:(group_id + 1) * group_cols], out_weight[group_id * group_cols:(group_id + 1) * group_cols], preferred_element_type=jnp.float32).astype(jnp.bfloat16)
        summed = summed + share_out.astype(jnp.float32)
    return summed.astype(jnp.bfloat16)
```

```python
import functools

import jax
import jax.numpy as jnp
from jax import lax
from jax.experimental import pallas as pl
from jax.experimental.pallas import tpu as pltpu
from jax.sharding import PartitionSpec as P

EPSILON = 1e-06
BF = jnp.bfloat16
F32 = jnp.float32
MESH = pl.DeviceIdType.MESH

BLK = 256
HALF = 128
NBLK = 8
HEADS = 4
DH = 128
COLS = HEADS * DH
TOK = NBLK * BLK
RING = 4
OUT = 2048
OROWS = TOK // RING
LOCAL = 3
REMOTE = 5
LEVELS = 20
ZERO_LANE = 127


def dot(a, b):
    return jnp.dot(a, b, preferred_element_type=F32)


def dot_t(a, b):
    return lax.dot_general(a, b, (((1,), (1,)), ((), ())), preferred_element_type=F32)


def dot_tl(a, b):
    return lax.dot_general(a, b, (((0,), (0,)), ((), ())), preferred_element_type=F32)


def lanes(w, lane, rows):
    return jnp.broadcast_to(w[:, lane : lane + 1], (rows, DH))


def kernel(
    idx_ref, tab_ref, q_hbm, k_hbm, v_hbm, w_hbm, o_hbm,
    qv, kv, vv, wb, wt, pick, leaf, near, tot, tsend, trecv, zr, yr, far, acc, nb, rb, of, ob,
    kvsem, qsem, wsem, osem,
    t_s, t_r, z_s, z_r, y_s, y_r, l_s, l_r,
    wx_s, wx_r, wz_s, wz_r, wy_s, wy_r, wd_s, wd_r, a_s, a_r,
):
    ctx = lax.axis_index("ctx")
    x = lax.axis_index("mp")
    c = lax.rem(ctx, 2)
    z = lax.rem(ctx // 2, RING)
    y = ctx // (2 * RING)

    def place(yy, zz, cc):
        return (yy * RING + zz) * 2 + cc

    def plus(p, d):
        return lax.rem(p + d, RING)

    partner = {"ctx": place(y, z, 1 - c), "mp": x}

    def zpeer(p):
        return {"ctx": place(y, p, c), "mp": x}

    def ypeer(p):
        return {"ctx": place(p, z, c), "mp": x}

    def xpeer(p):
        return {"ctx": ctx, "mp": p}

    def rcopy(src, dst, s, r, dev):
        return pltpu.make_async_remote_copy(
            src_ref=src, dst_ref=dst, send_sem=s, recv_sem=r, device_id=dev, device_id_type=MESH
        )

    barrier = pltpu.get_barrier_semaphore()
    pl.semaphore_signal(barrier, inc=1, device_id=partner, device_id_type=MESH)
    for d in (1, 2, 3):
        for dev in (zpeer(plus(z, d)), ypeer(plus(y, d)), xpeer(plus(x, d))):
            pl.semaphore_signal(barrier, inc=1, device_id=dev, device_id_type=MESH)

    def rows(n, size=BLK):
        return pl.ds(pl.multiple_of(n * size, size), size)

    def kload(n):
        return pltpu.make_async_copy(k_hbm.at[rows(n)], kv.at[rows(n)], kvsem.at[0, n])

    def vload(n):
        return pltpu.make_async_copy(v_hbm.at[rows(n)], vv.at[rows(n)], kvsem.at[1, n])

    qload = pltpu.make_async_copy(q_hbm, qv, qsem)
    wload = pltpu.make_async_copy(w_hbm, wb.at[x], wsem)
    for n in range(NBLK):
        kload(n).start()
        vload(n).start()
    wload.start()
    qload.start()

    table = tab_ref[...]
    hi = table.astype(BF)
    rest = table - hi.astype(F32)
    mid = rest.astype(BF)
    low = (rest - mid.astype(F32)).astype(BF)
    table3 = jnp.concatenate([hi, mid, low], axis=0)
    plan = lax.broadcasted_iota(jnp.int32, (16, DH), 0)
    for i in range(TOK // DH):
        hot = (jnp.broadcast_to(idx_ref[i : i + 1, :], (16, DH)) == plan).astype(F32).astype(BF)
        wt[i * DH : (i + 1) * DH, :] = dot_tl(jnp.concatenate([hot, hot, hot], axis=0), table3)
    tt = lax.broadcasted_iota(jnp.int32, (HALF, HALF), 0)
    ss = lax.broadcasted_iota(jnp.int32, (HALF, HALF), 1)
    apart = jnp.bitwise_xor(tt, ss)
    level = jnp.zeros((HALF, HALF), jnp.int32)
    for bit in range(7):
        level = level + (apart >= (1 << bit)).astype(jnp.int32)
    for h in range(HEADS):
        pick[h] = jnp.where(ss <= tt, level + h * LEVELS, ZERO_LANE)

    def leaf_body(n, carry):
        kload(n).wait()
        vload(n).wait()
        for h in range(HEADS):
            col = slice(h * DH, (h + 1) * DH)
            leaf[n, h] = dot_tl(kv[rows(n), col], vv[rows(n), col])
        return carry

    lax.fori_loop(0, NBLK, leaf_body, 0)
    for h in range(HEADS):
        total = leaf[0, h]
        for n in range(1, NBLK):
            total = total + leaf[n, h]
        tot[h] = total
        tsend[h] = total.astype(BF)

    pl.semaphore_wait(barrier, 10)
    tcopy = rcopy(tsend, trecv, t_s, t_r, partner)
    tcopy.start()

    def piece_a(quarter, p):
        return wb.at[quarter, rows(p, DH), pl.ds(pl.multiple_of(c * 1024, 1024), 512)]

    def piece_b(quarter, p):
        return wb.at[quarter, rows(p, DH), pl.ds(pl.multiple_of(c * 1024 + 512, 512), 512)]

    def wx_a(quarter, d):
        return rcopy(piece_a(quarter, z), piece_a(quarter, z), wx_s.at[d - 1, 0], wx_r.at[quarter, 0], xpeer(plus(x, d)))

    def wx_b(quarter, d):
        return rcopy(piece_b(quarter, y), piece_b(quarter, y), wx_s.at[d - 1, 1], wx_r.at[quarter, 1], xpeer(plus(x, d)))

    wload.wait()
    for d in (1, 3, 2):
        wx_a(x, d).start()
        wx_b(x, d).start()

    zero = jnp.zeros((DH, DH), BF)

    def near_body(h, carry):
        l0, l2, l4, l6 = leaf[0, h], leaf[2, h], leaf[4, h], leaf[6, h]
        p0 = l0 + leaf[1, h]
        p4 = l4 + leaf[5, h]
        f0 = p0 + (l2 + leaf[3, h])
        first = [l0, l2, l4, l6]
        for n in range(NBLK):
            near[n, h, 0:DH, :] = first[n // 2].astype(BF) if n & 1 else zero
            near[n, h, DH : 2 * DH, :] = (p4 if n & 4 else p0).astype(BF) if n & 2 else zero
            near[n, h, 2 * DH : 3 * DH, :] = f0.astype(BF) if n & 4 else zero
        return carry

    lax.fori_loop(0, HEADS, near_body, 0)
    qload.wait()

    half0 = c * 2

    def zcopy(src, d):
        return rcopy(zr.at[src], zr.at[src], z_s.at[d - 1], z_r.at[src], zpeer(plus(z, d)))

    def ycopy(src, d):
        return rcopy(yr.at[src], yr.at[src], y_s.at[d - 1], y_r.at[src], ypeer(plus(y, d)))

    def choose(cond, value):
        return jnp.where(cond, value, jnp.zeros_like(value))

    def exchange_z():
        tcopy.wait_recv()
        for h in range(HEADS):
            got = trecv[h]
            far[h, 0:DH, :] = choose(c == 1, got.astype(F32)).astype(BF)
        for i in range(2):
            zr[z, i] = (tot[half0 + i] + trecv[half0 + i].astype(F32)).astype(BF)
        for d in (1, 3, 2):
            zcopy(z, d).start()

    def exchange_y():
        for d in (1, 2, 3):
            zcopy(plus(z, d), d).wait_recv()
        for i in range(2):
            parts = [zr[p, i].astype(F32) for p in range(RING)]
            lower = zr[jnp.maximum(z - 1, 0), i].astype(F32)
            pair = parts[0] + parts[1]
            far[half0 + i, DH : 2 * DH, :] = choose(lax.rem(z, 2) == 1, lower).astype(BF)
            far[half0 + i, 2 * DH : 3 * DH, :] = choose(z >= 2, pair).astype(BF)
            yr[y, i] = (pair + (parts[2] + parts[3])).astype(BF)
        for d in (1, 2, 3):

            @pl.when(y + d < RING)
            def _():
                ycopy(y, d).start()

    def lcopy():
        mine = far.at[pl.ds(half0, 2), pl.ds(DH, 4 * DH)]
        return rcopy(mine, mine, l_s, l_r, partner)

    def exchange_end():
        for d in (1, 2, 3):

            @pl.when(y >= d)
            def _():
                ycopy(y - d, d).wait_recv()

        for i in range(2):
            lower = yr[jnp.maximum(y - 1, 0), i].astype(F32)
            pair = yr[0, i].astype(F32) + yr[1, i].astype(F32)
            far[half0 + i, 3 * DH : 4 * DH, :] = choose(lax.rem(y, 2) == 1, lower).astype(BF)
            far[half0 + i, 4 * DH : 5 * DH, :] = choose(y >= 2, pair).astype(BF)
        lcopy().start()

    def near_attention(n, carry):
        r = rows(n)
        w = wt[r, :]
        for h in range(HEADS):
            col = slice(h * DH, (h + 1) * DH)
            q, k, v = qv[r, col], kv[r, col], vv[r, col]
            at = pick[h]
            s_lo = dot_t(q[:HALF], k[:HALF])
            s_hi = dot_t(q[HALF:], k)
            p_lo = (s_lo * jnp.take_along_axis(w[:HALF], at, axis=1, mode="promise_in_bounds")).astype(BF)
            p_hi = jnp.concatenate(
                [
                    (s_hi[:, :HALF] * lanes(w[HALF:], h * LEVELS + 8, HALF)).astype(BF),
                    (s_hi[:, HALF:] * jnp.take_along_axis(w[HALF:], at, axis=1, mode="promise_in_bounds")).astype(BF),
                ],
                axis=1,
            )
            qf = q.astype(F32)
            ql = jnp.concatenate(
                [(qf * lanes(w, h * LEVELS + 9 + j, BLK)).astype(BF) for j in range(LOCAL)], axis=1
            )
            o = jnp.concatenate([dot(p_lo, v[:HALF]), dot(p_hi, v)], axis=0)
            acc[r, col] = o + dot(ql, near[n, h])

        @pl.when(n == 0)
        def _():
            exchange_z()

        @pl.when(n == 4)
        def _():
            exchange_y()

        return carry

    lax.fori_loop(0, NBLK, near_attention, 0)
    exchange_end()

    def wz(quarter, src, d):
        return rcopy(piece_a(quarter, src), piece_a(quarter, src), wz_s.at[quarter, d - 1], wz_r.at[quarter, src], zpeer(plus(z, d)))

    def wy(quarter, src, d):
        return rcopy(piece_b(quarter, src), piece_b(quarter, src), wy_s.at[quarter, d - 1], wy_r.at[quarter, src], ypeer(plus(y, d)))

    sources = (3, 1, 2)
    for e in sources:
        quarter = plus(x, e)
        wx_a(quarter, 1).wait_recv()
        wx_b(quarter, 1).wait_recv()
        for d in (1, 3, 2):
            wz(quarter, z, d).start()
            wy(quarter, y, d).start()

    lcopy().wait_recv()

    def acopy(src, part, d):
        return rcopy(
            nb.at[rows(2 * plus(src, d) + part)],
            rb.at[src, pl.ds(part * BLK, BLK)],
            a_s.at[d - 1, part],
            a_r.at[src, part],
            xpeer(plus(src, d)),
        )

    def finish(n):
        r = rows(n)
        w = wt[r, :]
        for h in range(HEADS):
            col = slice(h * DH, (h + 1) * DH)
            qf = qv[r, col].astype(F32)
            ql = jnp.concatenate(
                [(qf * lanes(w, h * LEVELS + 12 + j, BLK)).astype(BF) for j in range(REMOTE)], axis=1
            )
            o = acc[r, col] + dot(ql, far[h])
            ms = jnp.mean(o * o, axis=-1, keepdims=True)
            nb[r, col] = (o * lax.rsqrt(ms + EPSILON)).astype(BF)

    order = (1, 3, 2, 0)

    def finish_body(j, carry):
        part = j // RING
        i = lax.rem(j, RING)
        d = jnp.where(i == 0, 1, jnp.where(i == 1, 3, jnp.where(i == 2, 2, 0)))
        finish(2 * plus(x, d) + part)
        for p in range(2):
            for m, dd in enumerate(order[:3]):

                @pl.when(j == p * RING + m)
                def _():
                    acopy(x, p, dd).start()

        return carry

    lax.fori_loop(0, 2 * RING, finish_body, 0)

    NC = 256

    def ocopy(part, i):
        return pltpu.make_async_copy(
            ob.at[pl.ds(part * BLK, BLK), rows(i, NC)], o_hbm.at[pl.ds(part * BLK, BLK), rows(i, NC)], osem.at[part, i]
        )

    def project(quarter, part, own, last):
        rws = slice(part * BLK, (part + 1) * BLK)

        def body(i, carry):
            cl = rows(i, NC)
            a = nb[rows(2 * x + part), :] if own else rb[quarter, rws, :]
            s = dot(a, wb[quarter, :, cl])
            if not own:
                s = s + of[rws, cl]
            if last:
                ob[rws, cl] = s.astype(BF)
                ocopy(part, i).start()
            else:
                of[rws, cl] = s
            return carry

        lax.fori_loop(0, OUT // NC, body, 0)

    for part in range(2):
        project(x, part, True, False)

    def half_of(quarter):
        return wb.at[quarter, :, pl.ds(pl.multiple_of(c * 1024, 1024), 1024)]

    def wd(quarter, e):
        return rcopy(half_of(quarter), half_of(quarter), wd_s.at[e - 1], wd_r.at[quarter], partner)

    for e in sources:
        quarter = plus(x, e)
        for d in (1, 2, 3):
            wz(quarter, plus(z, d), d).wait_recv()
            wy(quarter, plus(y, d), d).wait_recv()
        wd(quarter, e).start()

    for part in range(2):
        for e in sources:
            quarter = plus(x, e)
            if part == 0:
                wd(quarter, e).wait_recv()
            acopy(quarter, part, RING - e).wait_recv()
            project(quarter, part, False, e == sources[-1])

    tcopy.wait_send()
    lcopy().wait_send()
    for d in (1, 2, 3):
        zcopy(z, d).wait_send()

        @pl.when(y + d < RING)
        def _():
            ycopy(y, d).wait_send()

        wx_a(x, d).wait_send()
        wx_b(x, d).wait_send()
        quarter = plus(x, d)
        for dd in (1, 2, 3):
            wz(quarter, z, dd).wait_send()
            wy(quarter, y, dd).wait_send()
        wd(quarter, d).wait_send()
        for part in range(2):
            acopy(x, part, d).wait_send()
    for part in range(2):
        for i in range(OUT // NC):
            ocopy(part, i).wait()


def body(queries, key_vectors, value_vectors, level_index, level_table, out_weight):
    table = jnp.pad(level_table.reshape(16, HEADS * LEVELS), ((0, 0), (0, DH - HEADS * LEVELS)))
    index = level_index.reshape(TOK // DH, DH)
    anyspec = pl.BlockSpec(memory_space=pl.ANY)
    vspec = pl.BlockSpec(memory_space=pltpu.VMEM)
    dma = pltpu.SemaphoreType.DMA
    scratch = [
        pltpu.VMEM((TOK, COLS), BF),
        pltpu.VMEM((TOK, COLS), BF),
        pltpu.VMEM((TOK, COLS), BF),
        pltpu.VMEM((RING, COLS, OUT), BF),
        pltpu.VMEM((TOK, DH), F32),
        pltpu.VMEM((HEADS, HALF, HALF), jnp.int32),
        pltpu.VMEM((NBLK, HEADS, DH, DH), F32),
        pltpu.VMEM((NBLK, HEADS, LOCAL * DH, DH), BF),
        pltpu.VMEM((HEADS, DH, DH), F32),
        pltpu.VMEM((HEADS, DH, DH), BF),
        pltpu.VMEM((HEADS, DH, DH), BF),
        pltpu.VMEM((RING, 2, DH, DH), BF),
        pltpu.VMEM((RING, 2, DH, DH), BF),
        pltpu.VMEM((HEADS, REMOTE * DH, DH), BF),
        pltpu.VMEM((TOK, COLS), F32),
        pltpu.VMEM((TOK, COLS), BF),
        pltpu.VMEM((RING, OROWS, COLS), BF),
        pltpu.VMEM((OROWS, OUT), F32),
        pltpu.VMEM((OROWS, OUT), BF),
        dma((2, NBLK)), dma, dma, dma((2, 8)),
        dma, dma, dma((3,)), dma((RING,)), dma((3,)), dma((RING,)), dma, dma,
        dma((3, 2)), dma((RING, 2)), dma((RING, 3)), dma((RING, RING)), dma((RING, 3)), dma((RING, RING)),
        dma((3,)), dma((RING,)), dma((3, 2)), dma((RING, 2)),
    ]
    return pl.pallas_call(
        kernel,
        out_shape=jax.ShapeDtypeStruct((OROWS, OUT), BF),
        in_specs=[vspec, vspec, anyspec, anyspec, anyspec, anyspec],
        out_specs=anyspec,
        scratch_shapes=scratch,
        compiler_params=pltpu.CompilerParams(
            collective_id=0, has_side_effects=True, vmem_limit_bytes=60 * 1024 * 1024
        ),
    )(index, table, queries, key_vectors, value_vectors, out_weight)


def solution(mesh):
    placed = (
        P("ctx", "mp"),
        P("ctx", "mp"),
        P("ctx", "mp"),
        P("ctx"),
        P(None, "mp", None),
        P("mp", None),
    )
    return jax.shard_map(
        body, mesh=mesh, in_specs=placed, out_specs=P(("ctx", "mp"), None), check_vma=False
    )
```

```python
import functools

import jax
import jax.numpy as jnp
from jax import lax
from jax.experimental import pallas as pl
from jax.experimental.pallas import tpu as pltpu
from jax.sharding import PartitionSpec as P

EPSILON = 1e-06
BF = jnp.bfloat16
F32 = jnp.float32
MESH = pl.DeviceIdType.MESH

BLK = 256
HALF = 128
NBLK = 8
HEADS = 4
DH = 128
COLS = HEADS * DH
TOK = NBLK * BLK
RING = 4
OUT = 2048
OROWS = TOK // RING
LOCAL = 3
REMOTE = 5
LEVELS = 20
ZERO_LANE = 127


def dot(a, b):
    return jnp.dot(a, b, preferred_element_type=F32)


def dot_t(a, b):
    return lax.dot_general(a, b, (((1,), (1,)), ((), ())), preferred_element_type=F32)


def dot_tl(a, b):
    return lax.dot_general(a, b, (((0,), (0,)), ((), ())), preferred_element_type=F32)


def lanes(w, lane, rows):
    return jnp.broadcast_to(w[:, lane : lane + 1], (rows, DH))


def kernel(
    idx_ref, tab_ref, q_hbm, k_hbm, v_hbm, w_hbm, o_ref,
    qv, kv, vv, wb, wt, pick, leaf, near, tot, tsend, trecv, zr, yr, far, acc, ql_far, nb, rb,
    kvsem, qsem, wsem,
    t_s, t_r, z_s, z_r, y_s, y_r, l_s, l_r,
    wx_s, wx_r, wz_s, wz_r, wy_s, wy_r, wd_s, wd_r, a_s, a_r,
):
    ctx = lax.axis_index("ctx")
    x = lax.axis_index("mp")
    c = lax.rem(ctx, 2)
    z = lax.rem(ctx // 2, RING)
    y = ctx // (2 * RING)

    def place(yy, zz, cc):
        return (yy * RING + zz) * 2 + cc

    def plus(p, d):
        return lax.rem(p + d, RING)

    partner = {"ctx": place(y, z, 1 - c), "mp": x}

    def zpeer(p):
        return {"ctx": place(y, p, c), "mp": x}

    def ypeer(p):
        return {"ctx": place(p, z, c), "mp": x}

    def xpeer(p):
        return {"ctx": ctx, "mp": p}

    def rcopy(src, dst, s, r, dev):
        return pltpu.make_async_remote_copy(
            src_ref=src, dst_ref=dst, send_sem=s, recv_sem=r, device_id=dev, device_id_type=MESH
        )

    barrier = pltpu.get_barrier_semaphore()
    pl.semaphore_signal(barrier, inc=1, device_id=partner, device_id_type=MESH)
    for d in (1, 2, 3):
        for dev in (zpeer(plus(z, d)), ypeer(plus(y, d)), xpeer(plus(x, d))):
            pl.semaphore_signal(barrier, inc=1, device_id=dev, device_id_type=MESH)

    def rows(n, size=BLK):
        return pl.ds(pl.multiple_of(n * size, size), size)

    def kload(n):
        return pltpu.make_async_copy(k_hbm.at[rows(n)], kv.at[rows(n)], kvsem.at[0, n])

    def vload(n):
        return pltpu.make_async_copy(v_hbm.at[rows(n)], vv.at[rows(n)], kvsem.at[1, n])

    qload = pltpu.make_async_copy(q_hbm, qv, qsem)
    wload = pltpu.make_async_copy(w_hbm, wb.at[x], wsem)
    for n in range(NBLK):
        kload(n).start()
        vload(n).start()
    wload.start()
    qload.start()

    def leaf_body(n, carry):
        kload(n).wait()
        vload(n).wait()
        for h in range(HEADS):
            col = slice(h * DH, (h + 1) * DH)
            leaf[n, h] = dot_tl(kv[rows(n), col], vv[rows(n), col])
        return carry

    lax.fori_loop(0, NBLK, leaf_body, 0)
    for h in range(HEADS):
        total = leaf[0, h]
        for n in range(1, NBLK):
            total = total + leaf[n, h]
        tot[h] = total
        tsend[h] = total.astype(BF)

    pl.semaphore_wait(barrier, 10)
    tcopy = rcopy(tsend, trecv, t_s, t_r, partner)
    tcopy.start()

    def piece_a(quarter, p):
        return wb.at[quarter, rows(p, DH), pl.ds(pl.multiple_of(c * 1024, 1024), 512)]

    def piece_b(quarter, p):
        return wb.at[quarter, rows(p, DH), pl.ds(pl.multiple_of(c * 1024 + 512, 512), 512)]

    def wx_a(quarter, d):
        return rcopy(piece_a(quarter, z), piece_a(quarter, z), wx_s.at[d - 1, 0], wx_r.at[quarter, 0], xpeer(plus(x, d)))

    def wx_b(quarter, d):
        return rcopy(piece_b(quarter, y), piece_b(quarter, y), wx_s.at[d - 1, 1], wx_r.at[quarter, 1], xpeer(plus(x, d)))

    wload.wait()
    for d in (1, 3, 2):
        wx_a(x, d).start()
        wx_b(x, d).start()

    table = jnp.concatenate(
        [tab_ref[:, h, :] for h in range(HEADS)] + [jnp.zeros((16, DH - HEADS * LEVELS), F32)], axis=1
    )
    hi = table.astype(BF)
    rest = table - hi.astype(F32)
    mid = rest.astype(BF)
    low = (rest - mid.astype(F32)).astype(BF)
    table3 = jnp.concatenate([hi, mid, low], axis=0)
    plan = lax.broadcasted_iota(jnp.int32, (16, DH), 0)
    for i in range(TOK // DH):
        hot = (jnp.broadcast_to(idx_ref[i : i + 1, :], (16, DH)) == plan).astype(F32).astype(BF)
        wt[i * DH : (i + 1) * DH, :] = dot_tl(jnp.concatenate([hot, hot, hot], axis=0), table3)
    tt = lax.broadcasted_iota(jnp.int32, (HALF, HALF), 0)
    ss = lax.broadcasted_iota(jnp.int32, (HALF, HALF), 1)
    apart = jnp.bitwise_xor(tt, ss)
    level = jnp.zeros((HALF, HALF), jnp.int32)
    for bit in range(7):
        level = level + (apart >= (1 << bit)).astype(jnp.int32)
    for h in range(HEADS):
        pick[h] = jnp.where(ss <= tt, level + h * LEVELS, ZERO_LANE)

    zero = jnp.zeros((DH, DH), BF)

    def near_body(h, carry):
        l0, l2, l4, l6 = leaf[0, h], leaf[2, h], leaf[4, h], leaf[6, h]
        p0 = l0 + leaf[1, h]
        p4 = l4 + leaf[5, h]
        f0 = p0 + (l2 + leaf[3, h])
        first = [l0, l2, l4, l6]
        for n in range(NBLK):
            near[n, h, 0:DH, :] = first[n // 2].astype(BF) if n & 1 else zero
            near[n, h, DH : 2 * DH, :] = (p4 if n & 4 else p0).astype(BF) if n & 2 else zero
            near[n, h, 2 * DH : 3 * DH, :] = f0.astype(BF) if n & 4 else zero
        return carry

    lax.fori_loop(0, HEADS, near_body, 0)
    qload.wait()

    half0 = c * 2

    def zcopy(src, d, i):
        return rcopy(zr.at[src, i], zr.at[src, i], z_s.at[d - 1, i], z_r.at[src, i], zpeer(plus(z, d)))

    def ycopy(src, d, i):
        return rcopy(yr.at[src, i], yr.at[src, i], y_s.at[d - 1, i], y_r.at[src, i], ypeer(plus(y, d)))

    def lcopy(i):
        mine = far.at[half0 + i, pl.ds(DH, 4 * DH)]
        return rcopy(mine, mine, l_s.at[i], l_r.at[i], partner)

    def choose(cond, value):
        return jnp.where(cond, value, jnp.zeros_like(value))

    def exchange_z():
        tcopy.wait_recv()
        for i in range(2):
            zr[z, i] = (tot[half0 + i] + trecv[half0 + i].astype(F32)).astype(BF)
            for d in (2, 1, 3):
                zcopy(z, d, i).start()
        for h in range(HEADS):
            far[h, 0:DH, :] = choose(c == 1, trecv[h].astype(F32)).astype(BF)

    def exchange_y(i):
        for d in (1, 2, 3):
            zcopy(plus(z, d), d, i).wait_recv()
        parts = [zr[p, i].astype(F32) for p in range(RING)]
        pair = parts[0] + parts[1]
        yr[y, i] = (pair + (parts[2] + parts[3])).astype(BF)
        for d in (2, 1, 3):

            @pl.when(y + d < RING)
            def _():
                ycopy(y, d, i).start()

        lower = zr[jnp.maximum(z - 1, 0), i].astype(F32)
        far[half0 + i, DH : 2 * DH, :] = choose(lax.rem(z, 2) == 1, lower).astype(BF)
        far[half0 + i, 2 * DH : 3 * DH, :] = choose(z >= 2, pair).astype(BF)

    def exchange_end(i):
        for d in (1, 2, 3):

            @pl.when(y >= d)
            def _():
                ycopy(y - d, d, i).wait_recv()

        lower = yr[jnp.maximum(y - 1, 0), i].astype(F32)
        pair = yr[0, i].astype(F32) + yr[1, i].astype(F32)
        far[half0 + i, 3 * DH : 4 * DH, :] = choose(lax.rem(y, 2) == 1, lower).astype(BF)
        far[half0 + i, 4 * DH : 5 * DH, :] = choose(y >= 2, pair).astype(BF)
        lcopy(i).start()

    exchange_z()

    def near_attention(n, carry):
        r = rows(n)
        w = wt[r, :]
        for h in range(HEADS):
            col = slice(h * DH, (h + 1) * DH)
            q, k, v = qv[r, col], kv[r, col], vv[r, col]
            at = pick[h]
            s_lo = dot_t(q[:HALF], k[:HALF])
            s_hi = dot_t(q[HALF:], k)
            p_lo = (s_lo * jnp.take_along_axis(w[:HALF], at, axis=1, mode="promise_in_bounds")).astype(BF)
            p_hi = jnp.concatenate(
                [
                    (s_hi[:, :HALF] * lanes(w[HALF:], h * LEVELS + 8, HALF)).astype(BF),
                    (s_hi[:, HALF:] * jnp.take_along_axis(w[HALF:], at, axis=1, mode="promise_in_bounds")).astype(BF),
                ],
                axis=1,
            )
            qf = q.astype(F32)
            ql = jnp.concatenate(
                [(qf * lanes(w, h * LEVELS + 9 + j, BLK)).astype(BF) for j in range(LOCAL)], axis=1
            )
            o = jnp.concatenate([dot(p_lo, v[:HALF]), dot(p_hi, v)], axis=0)
            acc[r, col] = o + dot(ql, near[n, h])
            for j in range(REMOTE):
                ql_far[r, (h * REMOTE + j) * DH : (h * REMOTE + j + 1) * DH] = (
                    qf * lanes(w, h * LEVELS + 12 + j, BLK)
                ).astype(BF)

        for at_n, hook in hooks:

            @pl.when(n == at_n)
            def _():
                hook()

        return carry

    def wz(quarter, src, d):
        return rcopy(piece_a(quarter, src), piece_a(quarter, src), wz_s.at[quarter, d - 1], wz_r.at[quarter, src], zpeer(plus(z, d)))

    def wy(quarter, src, d):
        return rcopy(piece_b(quarter, src), piece_b(quarter, src), wy_s.at[quarter, d - 1], wy_r.at[quarter, src], ypeer(plus(y, d)))

    sources = (3, 1, 2)

    def send_wz(es):
        for e in es:
            wx_a(plus(x, e), 1).wait_recv()
            for d in (2, 1, 3):
                wz(plus(x, e), z, d).start()

    hooks = (
        (3, lambda: exchange_y(0)),
        (4, lambda: exchange_y(1)),
        (6, lambda: send_wz((3, 1))),
        (7, lambda: exchange_end(0)),
    )
    lax.fori_loop(0, NBLK, near_attention, 0)
    exchange_end(1)
    send_wz((2,))
    for e in sources:
        wx_b(plus(x, e), 1).wait_recv()
        for d in (2, 1, 3):
            wy(plus(x, e), y, d).start()

    def acopy(src, slot, d):
        own = lax.rem(slot + c, 2)
        block = 2 * plus(src, d)
        if slot < 2:
            cols = pl.ds(pl.multiple_of(own * 2 * DH, 2 * DH), 2 * DH)
            here = nb.at[rows(block), cols]
            there = rb.at[src, pl.ds(0, BLK), cols]
        else:
            here = nb.at[rows(2 * block + slot, HALF)]
            there = rb.at[src, pl.ds(slot * HALF, HALF)]
        return rcopy(here, there, a_s.at[d - 1, slot], a_r.at[src, slot], xpeer(plus(src, d)))

    def finish(n, pair):
        r = rows(n)
        for i in range(2):
            h = 2 * pair + i
            col = pl.ds(pl.multiple_of(h * DH, DH), DH)
            wide = pl.ds(pl.multiple_of(h * REMOTE * DH, DH), REMOTE * DH)
            o = acc[r, col] + dot(ql_far[r, wide], far[h])
            ms = jnp.mean(o * o, axis=-1, keepdims=True)
            nb[r, col] = (o * lax.rsqrt(ms + EPSILON)).astype(BF)

    order = (2, 1, 3)

    def offset(i):
        return jnp.where(i == 0, order[0], jnp.where(i == 1, order[1], jnp.where(i == 2, order[2], 0)))

    def send_slots(i, slots):
        for m, d in enumerate(order):

            @pl.when(i == m)
            def _():
                for slot in slots:
                    acopy(x, slot, d).start()

    def early(slot):
        def body(i, carry):
            finish(2 * plus(x, offset(i)), lax.rem(slot + c, 2))
            send_slots(i, (slot,))
            return carry

        lax.fori_loop(0, 3, body, 0)

    def late(i, carry):
        n = 2 * plus(x, offset(i)) + 1
        finish(n, 0)
        finish(n, 1)
        send_slots(i, (2, 3))
        return carry

    early(0)
    for i in range(2):
        theirs = far.at[2 * (1 - c) + i, pl.ds(DH, 4 * DH)]
        rcopy(theirs, theirs, l_s.at[i], l_r.at[i], partner).wait_recv()
    early(1)
    lax.fori_loop(0, 4, late, 0)
    finish(2 * x, 0)
    finish(2 * x, 1)

    NC = 512

    def project(row, size):
        rws = pl.ds(row, size)

        def body(i, carry):
            cl = rows(i, NC)
            s = dot(nb[pl.ds(pl.multiple_of(x * OROWS, OROWS) + row, size), :], wb[x, :, cl])
            for e in sources:
                s = s + dot(rb[plus(x, e), rws, :], wb[plus(x, e), :, cl])
            o_ref[rws, cl] = s.astype(BF)
            return carry

        lax.fori_loop(0, OUT // NC, body, 0)

    def half_of(quarter):
        return wb.at[quarter, :, pl.ds(pl.multiple_of(c * 1024, 1024), 1024)]

    def wd(quarter, e):
        return rcopy(half_of(quarter), half_of(quarter), wd_s.at[e - 1], wd_r.at[quarter], partner)

    for e in sources:
        quarter = plus(x, e)
        for d in (1, 2, 3):
            wz(quarter, plus(z, d), d).wait_recv()
            wy(quarter, plus(y, d), d).wait_recv()
        wd(quarter, e).start()

    for e in sources:
        wd(plus(x, e), e).wait_recv()
    for slot in range(4):
        for e in sources:
            acopy(plus(x, e), slot, RING - e).wait_recv()
        if slot == 1:
            project(0, BLK)
        elif slot > 1:
            project(slot * HALF, HALF)

    tcopy.wait_send()
    for i in range(2):
        lcopy(i).wait_send()
    for d in (1, 2, 3):
        for i in range(2):
            zcopy(z, d, i).wait_send()

            @pl.when(y + d < RING)
            def _():
                ycopy(y, d, i).wait_send()

        wx_a(x, d).wait_send()
        wx_b(x, d).wait_send()
        quarter = plus(x, d)
        for dd in (1, 2, 3):
            wz(quarter, z, dd).wait_send()
            wy(quarter, y, dd).wait_send()
        wd(quarter, d).wait_send()
        for slot in range(4):
            acopy(x, slot, d).wait_send()


def body(queries, key_vectors, value_vectors, level_index, level_table, out_weight):
    index = level_index.reshape(TOK // DH, DH)
    anyspec = pl.BlockSpec(memory_space=pl.ANY)
    vspec = pl.BlockSpec(memory_space=pltpu.VMEM)
    dma = pltpu.SemaphoreType.DMA
    scratch = [
        pltpu.VMEM((TOK, COLS), BF),
        pltpu.VMEM((TOK, COLS), BF),
        pltpu.VMEM((TOK, COLS), BF),
        pltpu.VMEM((RING, COLS, OUT), BF),
        pltpu.VMEM((TOK, DH), F32),
        pltpu.VMEM((HEADS, HALF, HALF), jnp.int32),
        pltpu.VMEM((NBLK, HEADS, DH, DH), F32),
        pltpu.VMEM((NBLK, HEADS, LOCAL * DH, DH), BF),
        pltpu.VMEM((HEADS, DH, DH), F32),
        pltpu.VMEM((HEADS, DH, DH), BF),
        pltpu.VMEM((HEADS, DH, DH), BF),
        pltpu.VMEM((RING, 2, DH, DH), BF),
        pltpu.VMEM((RING, 2, DH, DH), BF),
        pltpu.VMEM((HEADS, REMOTE * DH, DH), BF),
        pltpu.VMEM((TOK, COLS), F32),
        pltpu.VMEM((TOK, HEADS * REMOTE * DH), BF),
        pltpu.VMEM((TOK, COLS), BF),
        pltpu.VMEM((RING, OROWS, COLS), BF),
        dma((2, NBLK)), dma, dma,
        dma, dma, dma((3, 2)), dma((RING, 2)), dma((3, 2)), dma((RING, 2)), dma((2,)), dma((2,)),
        dma((3, 2)), dma((RING, 2)), dma((RING, 3)), dma((RING, RING)), dma((RING, 3)), dma((RING, RING)),
        dma((3,)), dma((RING,)), dma((3, 4)), dma((RING, 4)),
    ]
    return pl.pallas_call(
        kernel,
        out_shape=pltpu.VMEM((OROWS, OUT), BF),
        in_specs=[vspec, vspec, anyspec, anyspec, anyspec, anyspec],
        out_specs=vspec,
        scratch_shapes=scratch,
        compiler_params=pltpu.CompilerParams(
            collective_id=0, has_side_effects=True, vmem_limit_bytes=56 * 1024 * 1024
        ),
    )(index, level_table, queries, key_vectors, value_vectors, out_weight)


def solution(mesh):
    placed = (
        P("ctx", "mp"),
        P("ctx", "mp"),
        P("ctx", "mp"),
        P("ctx"),
        P(None, "mp", None),
        P("mp", None),
    )
    return jax.shard_map(
        body, mesh=mesh, in_specs=placed, out_specs=P(("ctx", "mp"), None), check_vma=False
    )
```

```python
import functools

import jax
import jax.numpy as jnp
from jax import lax
from jax.experimental import pallas as pl
from jax.experimental.pallas import tpu as pltpu
from jax.sharding import PartitionSpec as P

EPSILON = 1e-06
BF = jnp.bfloat16
F32 = jnp.float32
MESH = pl.DeviceIdType.MESH

BLK = 256
HALF = 128
NBLK = 8
HEADS = 4
DH = 128
COLS = HEADS * DH
TOK = NBLK * BLK
RING = 4
OUT = 2048
OROWS = TOK // RING
LOCAL = 3
REMOTE = 5
LEVELS = 20
ZERO_LANE = 127


def dot(a, b):
    return jnp.dot(a, b, preferred_element_type=F32)


def dot_t(a, b):
    return lax.dot_general(a, b, (((1,), (1,)), ((), ())), preferred_element_type=F32)


def dot_tl(a, b):
    return lax.dot_general(a, b, (((0,), (0,)), ((), ())), preferred_element_type=F32)


GATHER = lax.GatherDimensionNumbers(
    offset_dims=(),
    collapsed_slice_dims=(1,),
    start_index_map=(1,),
    operand_batching_dims=(0,),
    start_indices_batching_dims=(0,),
)


def pick_lanes(w, at):
    return lax.gather(w, at[..., None], GATHER, (1, 1), mode=lax.GatherScatterMode.PROMISE_IN_BOUNDS)


def beside(*parts):
    return jnp.concatenate(parts, axis=1)


def stacked(*parts):
    return jnp.concatenate(parts, axis=0)


def lanes(w, lane, rows):
    return jnp.broadcast_to(w[:, lane : lane + 1], (rows, DH))


def kernel(
    idx_ref, tab_ref, q_hbm, k_hbm, v_hbm, w_hbm, o_ref,
    qv, kv, vv, wb, wt, pick, leaf, near, tot, tsend, trecv, zr, yr, far, acc, ql_far, nb, rb,
    kvsem, qsem, wsem,
    t_s, t_r, z_s, z_r, y_s, y_r, l_s, l_r,
    wx_s, wx_r, wz_s, wz_r, wy_s, wy_r, wd_s, wd_r, a_s, a_r,
):
    ctx = lax.axis_index("ctx")
    x = lax.axis_index("mp")
    c = lax.rem(ctx, 2)
    z = lax.rem(ctx // 2, RING)
    y = ctx // (2 * RING)

    def place(yy, zz, cc):
        return (yy * RING + zz) * 2 + cc

    def plus(p, d):
        return lax.rem(p + d, RING)

    partner = {"ctx": place(y, z, 1 - c), "mp": x}

    def zpeer(p):
        return {"ctx": place(y, p, c), "mp": x}

    def ypeer(p):
        return {"ctx": place(p, z, c), "mp": x}

    def xpeer(p):
        return {"ctx": ctx, "mp": p}

    def rcopy(src, dst, s, r, dev):
        return pltpu.make_async_remote_copy(
            src_ref=src, dst_ref=dst, send_sem=s, recv_sem=r, device_id=dev, device_id_type=MESH
        )

    barrier = pltpu.get_barrier_semaphore()
    pl.semaphore_signal(barrier, inc=1, device_id=partner, device_id_type=MESH)
    for d in (1, 2, 3):
        for dev in (zpeer(plus(z, d)), ypeer(plus(y, d)), xpeer(plus(x, d))):
            pl.semaphore_signal(barrier, inc=1, device_id=dev, device_id_type=MESH)

    def rows(n, size=BLK):
        return pl.ds(pl.multiple_of(n * size, size), size)

    def kload(n):
        return pltpu.make_async_copy(k_hbm.at[rows(n)], kv.at[rows(n)], kvsem.at[0, n])

    def vload(n):
        return pltpu.make_async_copy(v_hbm.at[rows(n)], vv.at[rows(n)], kvsem.at[1, n])

    qload = pltpu.make_async_copy(q_hbm, qv, qsem)
    wload = pltpu.make_async_copy(w_hbm, wb.at[x], wsem)
    for n in range(NBLK):
        kload(n).start()
        vload(n).start()

    def leaf_body(n, carry):
        kload(n).wait()
        vload(n).wait()

        @pl.when(n == 3)
        def _():
            wload.start()
            qload.start()

        for h in range(HEADS):
            col = slice(h * DH, (h + 1) * DH)
            leaf[n, h] = dot_tl(kv[rows(n), col], vv[rows(n), col])
        return carry

    lax.fori_loop(0, NBLK, leaf_body, 0)
    for h in range(HEADS):
        total = leaf[0, h]
        for n in range(1, NBLK):
            total = total + leaf[n, h]
        tot[h] = total
        tsend[h] = total.astype(BF)

    pl.semaphore_wait(barrier, 10)
    tcopy = rcopy(tsend, trecv, t_s, t_r, partner)
    tcopy.start()

    def piece_a(quarter, p):
        return wb.at[quarter, rows(p, DH), pl.ds(pl.multiple_of(c * 1024, 1024), 512)]

    def piece_b(quarter, p):
        return wb.at[quarter, rows(p, DH), pl.ds(pl.multiple_of(c * 1024 + 512, 512), 512)]

    def wx_a(quarter, d):
        return rcopy(piece_a(quarter, z), piece_a(quarter, z), wx_s.at[d - 1, 0], wx_r.at[quarter, 0], xpeer(plus(x, d)))

    def wx_b(quarter, d):
        return rcopy(piece_b(quarter, y), piece_b(quarter, y), wx_s.at[d - 1, 1], wx_r.at[quarter, 1], xpeer(plus(x, d)))

    wload.wait()
    for d in (1, 3, 2):
        wx_a(x, d).start()
        wx_b(x, d).start()

    table = jnp.concatenate(
        [tab_ref[:, h, :] for h in range(HEADS)] + [jnp.zeros((16, DH - HEADS * LEVELS), F32)], axis=1
    )
    hi = table.astype(BF)
    rest = table - hi.astype(F32)
    mid = rest.astype(BF)
    low = (rest - mid.astype(F32)).astype(BF)
    table3 = jnp.concatenate([hi, mid, low], axis=0)
    plan = lax.broadcasted_iota(jnp.int32, (16, DH), 0)
    for i in range(TOK // DH):
        hot = (jnp.broadcast_to(idx_ref[i : i + 1, :], (16, DH)) == plan).astype(F32).astype(BF)
        wt[i * DH : (i + 1) * DH, :] = dot_tl(jnp.concatenate([hot, hot, hot], axis=0), table3)
    tt = lax.broadcasted_iota(jnp.int32, (HALF, HALF), 0)
    ss = lax.broadcasted_iota(jnp.int32, (HALF, HALF), 1)
    apart = jnp.bitwise_xor(tt, ss)
    level = jnp.zeros((HALF, HALF), jnp.int32)
    for bit in range(7):
        level = level + (apart >= (1 << bit)).astype(jnp.int32)
    for h in range(HEADS):
        pick[h] = jnp.where(ss <= tt, level + h * LEVELS, ZERO_LANE)

    zero = jnp.zeros((DH, DH), BF)

    for h in range(HEADS):
        l0, l2, l4, l6 = leaf[0, h], leaf[2, h], leaf[4, h], leaf[6, h]
        p0 = l0 + leaf[1, h]
        p4 = l4 + leaf[5, h]
        f0 = p0 + (l2 + leaf[3, h])
        near[h, 0] = zero
        for i, node in enumerate((l0, l2, l4, l6, p0, p4, f0)):
            near[h, 1 + i] = node.astype(BF)
    for p in range(2):
        far[p, 0 : REMOTE * DH, DH:] = jnp.zeros((REMOTE * DH, DH), BF)
        far[p, REMOTE * DH :, :DH] = jnp.zeros((REMOTE * DH, DH), BF)
    qload.wait()

    half0 = c * 2

    def far_at(pair, i, first, count):
        return far.at[pair, pl.ds((i * REMOTE + first) * DH, count * DH), pl.ds(i * DH, DH)]

    def zcopy(src, d, i):
        return rcopy(zr.at[src, i], zr.at[src, i], z_s.at[d - 1, i], z_r.at[src, i], zpeer(plus(z, d)))

    def ycopy(src, d, i):
        return rcopy(yr.at[src, i], yr.at[src, i], y_s.at[d - 1, i], y_r.at[src, i], ypeer(plus(y, d)))

    def lcopy(i):
        mine = far_at(c, i, 1, 4)
        return rcopy(mine, mine, l_s.at[i], l_r.at[i], partner)

    def choose(cond, value):
        return jnp.where(cond, value, jnp.zeros_like(value))

    def exchange_z():
        tcopy.wait_recv()
        for i in range(2):
            zr[z, i] = (tot[half0 + i] + trecv[half0 + i].astype(F32)).astype(BF)
            for d in (2, 1, 3):
                zcopy(z, d, i).start()
        for h in range(HEADS):
            far_at(h // 2, h % 2, 0, 1)[...] = choose(c == 1, trecv[h].astype(F32)).astype(BF)

    def exchange_y(i):
        for d in (1, 2, 3):
            zcopy(plus(z, d), d, i).wait_recv()
        parts = [zr[p, i].astype(F32) for p in range(RING)]
        pair = parts[0] + parts[1]
        yr[y, i] = (pair + (parts[2] + parts[3])).astype(BF)
        for d in (2, 1, 3):

            @pl.when(y + d < RING)
            def _():
                ycopy(y, d, i).start()

        lower = zr[jnp.maximum(z - 1, 0), i].astype(F32)
        far_at(c, i, 1, 1)[...] = choose(lax.rem(z, 2) == 1, lower).astype(BF)
        far_at(c, i, 2, 1)[...] = choose(z >= 2, pair).astype(BF)

    def exchange_end(i):
        for d in (1, 2, 3):

            @pl.when(y >= d)
            def _():
                ycopy(y - d, d, i).wait_recv()

        lower = yr[jnp.maximum(y - 1, 0), i].astype(F32)
        pair = yr[0, i].astype(F32) + yr[1, i].astype(F32)
        far_at(c, i, 3, 1)[...] = choose(lax.rem(y, 2) == 1, lower).astype(BF)
        far_at(c, i, 4, 1)[...] = choose(y >= 2, pair).astype(BF)
        lcopy(i).start()

    exchange_z()

    def near_attention(n, carry):
        r = rows(n)
        w = wt[r, :]
        w16 = w.astype(BF)
        which = (
            jnp.where(lax.rem(n, 2) == 1, 1 + n // 2, 0),
            jnp.where(lax.rem(n // 2, 2) == 1, jnp.where(n >= 4, 6, 5), 0),
            jnp.where(n >= 4, 7, 0),
        )
        z_lo, z_hi = jnp.zeros((HALF, DH), BF), jnp.zeros((BLK, DH), BF)
        for p in range(2):
            low, high, near_q, values = [], [], [], []
            for h in (2 * p, 2 * p + 1):
                col = slice(h * DH, (h + 1) * DH)
                q, k, v = qv[r, col], kv[r, col], vv[r, col]
                at = pick[h]
                s_lo = dot_t(q[:HALF], k[:HALF])
                s_hi = dot_t(q[HALF:], k)
                low.append((s_lo * pick_lanes(w[:HALF], at)).astype(BF))
                high.append((s_hi[:, :HALF] * lanes(w16[HALF:], h * LEVELS + 8, HALF).astype(F32)).astype(BF))
                high.append((s_hi[:, HALF:] * pick_lanes(w[HALF:], at)).astype(BF))
                for j in range(LOCAL):
                    near_q.append(q * lanes(w16, h * LEVELS + 9 + j, BLK))
                for j in range(REMOTE):
                    ql_far[r, (h * REMOTE + j) * DH : (h * REMOTE + j + 1) * DH] = q * lanes(
                        w16, h * LEVELS + 12 + j, BLK
                    )
                values.append(v)
            va, vb = values
            nodes_a, nodes_b = ([near[h, t] for t in which] for h in (2 * p, 2 * p + 1))
            states = stacked(
                *[beside(t, zero) for t in nodes_a],
                *[beside(zero, t) for t in nodes_b],
            )
            pair = slice(2 * p * DH, 2 * (p + 1) * DH)
            acc[rows(2 * n, HALF), pair] = dot(
                beside(*low, *[t[:HALF] for t in near_q]),
                stacked(beside(va[:HALF], z_lo), beside(z_lo, vb[:HALF]), states),
            )
            acc[rows(2 * n + 1, HALF), pair] = dot(
                beside(*high, *[t[HALF:] for t in near_q]),
                stacked(beside(va, z_hi), beside(z_hi, vb), states),
            )

        for at_n, hook in hooks:

            @pl.when(n == at_n)
            def _():
                hook()

        return carry

    def wz(quarter, src, d):
        return rcopy(piece_a(quarter, src), piece_a(quarter, src), wz_s.at[quarter, d - 1], wz_r.at[quarter, src], zpeer(plus(z, d)))

    def wy(quarter, src, d):
        return rcopy(piece_b(quarter, src), piece_b(quarter, src), wy_s.at[quarter, d - 1], wy_r.at[quarter, src], ypeer(plus(y, d)))

    sources = (3, 1, 2)

    def send_wz(es):
        for e in es:
            wx_a(plus(x, e), 1).wait_recv()
            for d in (2, 1, 3):
                wz(plus(x, e), z, d).start()

    hooks = (
        (5, lambda: exchange_y(0)),
        (7, lambda: exchange_y(1)),
    )
    lax.fori_loop(0, NBLK, near_attention, 0)
    send_wz((3, 1))
    exchange_end(0)
    exchange_end(1)
    send_wz((2,))
    for e in sources:
        wx_b(plus(x, e), 1).wait_recv()
        for d in (2, 1, 3):
            wy(plus(x, e), y, d).start()

    def acopy(src, slot, d):
        own = lax.rem(slot + c, 2)
        block = 2 * plus(src, d)
        if slot < 2:
            cols = pl.ds(pl.multiple_of(own * 2 * DH, 2 * DH), 2 * DH)
            here = nb.at[rows(block), cols]
            there = rb.at[src, pl.ds(0, BLK), cols]
        else:
            here = nb.at[rows(2 * block + slot, HALF)]
            there = rb.at[src, pl.ds(slot * HALF, HALF)]
        return rcopy(here, there, a_s.at[d - 1, slot], a_r.at[src, slot], xpeer(plus(src, d)))

    def finish(n, pair):
        r = rows(n)
        col = pl.ds(pl.multiple_of(pair * 2 * DH, 2 * DH), 2 * DH)
        wide = pl.ds(pl.multiple_of(pair * 2 * REMOTE * DH, 2 * REMOTE * DH), 2 * REMOTE * DH)
        o = acc[r, col] + dot(ql_far[r, wide], far[pair])
        done = []
        for t in (o[:, :DH], o[:, DH:]):
            ms = jnp.mean(t * t, axis=-1, keepdims=True)
            done.append((t * lax.rsqrt(ms + EPSILON)).astype(BF))
        nb[r, col] = beside(*done)

    order = (2, 1, 3)

    def offset(i):
        return jnp.where(i == 0, order[0], jnp.where(i == 1, order[1], jnp.where(i == 2, order[2], 0)))

    def send_slots(i, slots):
        for m, d in enumerate(order):

            @pl.when(i == m)
            def _():
                for slot in slots:
                    acopy(x, slot, d).start()

    def early(slot):
        def body(i, carry):
            finish(2 * plus(x, offset(i)), lax.rem(slot + c, 2))
            send_slots(i, (slot,))
            return carry

        lax.fori_loop(0, 3, body, 0)

    def late(i, carry):
        n = 2 * plus(x, offset(i)) + 1
        finish(n, 0)
        finish(n, 1)
        send_slots(i, (2, 3))
        return carry

    early(0)
    for i in range(2):
        theirs = far_at(1 - c, i, 1, 4)
        rcopy(theirs, theirs, l_s.at[i], l_r.at[i], partner).wait_recv()
    early(1)
    lax.fori_loop(0, 4, late, 0)
    finish(2 * x, 0)
    finish(2 * x, 1)

    NC = 512

    def project(row, size):
        rws = pl.ds(row, size)

        def body(i, carry):
            cl = rows(i, NC)
            s = dot(nb[pl.ds(pl.multiple_of(x * OROWS, OROWS) + row, size), :], wb[x, :, cl])
            for e in sources:
                s = s + dot(rb[plus(x, e), rws, :], wb[plus(x, e), :, cl])
            o_ref[rws, cl] = s.astype(BF)
            return carry

        lax.fori_loop(0, OUT // NC, body, 0)

    def half_of(quarter):
        return wb.at[quarter, :, pl.ds(pl.multiple_of(c * 1024, 1024), 1024)]

    def wd(quarter, e):
        return rcopy(half_of(quarter), half_of(quarter), wd_s.at[e - 1], wd_r.at[quarter], partner)

    for e in sources:
        quarter = plus(x, e)
        for d in (1, 2, 3):
            wz(quarter, plus(z, d), d).wait_recv()
            wy(quarter, plus(y, d), d).wait_recv()
        wd(quarter, e).start()

    for e in sources:
        wd(plus(x, e), e).wait_recv()
    for slot in range(4):
        for e in sources:
            acopy(plus(x, e), slot, RING - e).wait_recv()
        if slot == 1:
            project(0, BLK)
        elif slot > 1:
            project(slot * HALF, HALF)

    tcopy.wait_send()
    for i in range(2):
        lcopy(i).wait_send()
    for d in (1, 2, 3):
        for i in range(2):
            zcopy(z, d, i).wait_send()

            @pl.when(y + d < RING)
            def _():
                ycopy(y, d, i).wait_send()

        wx_a(x, d).wait_send()
        wx_b(x, d).wait_send()
        quarter = plus(x, d)
        for dd in (1, 2, 3):
            wz(quarter, z, dd).wait_send()
            wy(quarter, y, dd).wait_send()
        wd(quarter, d).wait_send()
        for slot in range(4):
            acopy(x, slot, d).wait_send()


def body(queries, key_vectors, value_vectors, level_index, level_table, out_weight):
    index = level_index.reshape(TOK // DH, DH)
    anyspec = pl.BlockSpec(memory_space=pl.ANY)
    vspec = pl.BlockSpec(memory_space=pltpu.VMEM)
    dma = pltpu.SemaphoreType.DMA
    scratch = [
        pltpu.VMEM((TOK, COLS), BF),
        pltpu.VMEM((TOK, COLS), BF),
        pltpu.VMEM((TOK, COLS), BF),
        pltpu.VMEM((RING, COLS, OUT), BF),
        pltpu.VMEM((TOK, DH), F32),
        pltpu.VMEM((HEADS, HALF, HALF), jnp.int32),
        pltpu.VMEM((NBLK, HEADS, DH, DH), F32),
        pltpu.VMEM((HEADS, 8, DH, DH), BF),
        pltpu.VMEM((HEADS, DH, DH), F32),
        pltpu.VMEM((HEADS, DH, DH), BF),
        pltpu.VMEM((HEADS, DH, DH), BF),
        pltpu.VMEM((RING, 2, DH, DH), BF),
        pltpu.VMEM((RING, 2, DH, DH), BF),
        pltpu.VMEM((2, 2 * REMOTE * DH, 2 * DH), BF),
        pltpu.VMEM((TOK, COLS), F32),
        pltpu.VMEM((TOK, HEADS * REMOTE * DH), BF),
        pltpu.VMEM((TOK, COLS), BF),
        pltpu.VMEM((RING, OROWS, COLS), BF),
        dma((2, NBLK)), dma, dma,
        dma, dma, dma((3, 2)), dma((RING, 2)), dma((3, 2)), dma((RING, 2)), dma((2,)), dma((2,)),
        dma((3, 2)), dma((RING, 2)), dma((RING, 3)), dma((RING, RING)), dma((RING, 3)), dma((RING, RING)),
        dma((3,)), dma((RING,)), dma((3, 4)), dma((RING, 4)),
    ]
    return pl.pallas_call(
        kernel,
        out_shape=pltpu.VMEM((OROWS, OUT), BF),
        in_specs=[vspec, vspec, anyspec, anyspec, anyspec, anyspec],
        out_specs=vspec,
        scratch_shapes=scratch,
        compiler_params=pltpu.CompilerParams(
            collective_id=0, has_side_effects=True, vmem_limit_bytes=56 * 1024 * 1024
        ),
    )(index, level_table, queries, key_vectors, value_vectors, out_weight)


def solution(mesh):
    placed = (
        P("ctx", "mp"),
        P("ctx", "mp"),
        P("ctx", "mp"),
        P("ctx"),
        P(None, "mp", None),
        P("mp", None),
    )
    return jax.shard_map(
        body, mesh=mesh, in_specs=placed, out_specs=P(("ctx", "mp"), None), check_vma=False
    )
```

```python
import functools

import jax
import jax.numpy as jnp
from jax import lax
from jax.experimental import pallas as pl
from jax.experimental.pallas import tpu as pltpu
from jax.sharding import PartitionSpec as P

EPSILON = 1e-06
BF = jnp.bfloat16
F32 = jnp.float32
MESH = pl.DeviceIdType.MESH

BLK = 256
HALF = 128
NBLK = 8
HEADS = 4
DH = 128
COLS = HEADS * DH
TOK = NBLK * BLK
RING = 4
OUT = 2048
OROWS = TOK // RING
LOCAL = 3
REMOTE = 5
LEVELS = 20
ZERO_LANE = 127


def dot(a, b):
    return jnp.dot(a, b, preferred_element_type=F32)


def dot_t(a, b):
    return lax.dot_general(a, b, (((1,), (1,)), ((), ())), preferred_element_type=F32)


def dot_tl(a, b):
    return lax.dot_general(a, b, (((0,), (0,)), ((), ())), preferred_element_type=F32)


GATHER = lax.GatherDimensionNumbers(
    offset_dims=(),
    collapsed_slice_dims=(1,),
    start_index_map=(1,),
    operand_batching_dims=(0,),
    start_indices_batching_dims=(0,),
)


def pick_lanes(w, at):
    return lax.gather(w, at[..., None], GATHER, (1, 1), mode=lax.GatherScatterMode.PROMISE_IN_BOUNDS)


def beside(*parts):
    return jnp.concatenate(parts, axis=1)


def stacked(*parts):
    return jnp.concatenate(parts, axis=0)


def lanes(w, lane, rows):
    return jnp.broadcast_to(w[:, lane : lane + 1], (rows, DH))


def kernel(
    idx_ref, tab_ref, q_hbm, k_hbm, v_hbm, w_hbm, o_ref,
    qv, kv, vv, wb, wt, pick, leaf, near, tot, tsend, trecv, zr, yr, far, acc, ql_far, nb, rb, own,
    kvsem, qsem, wsem,
    t_s, t_r, z_s, z_r, y_s, y_r, l_s, l_r,
    wx_s, wx_r, wz_s, wz_r, wy_s, wy_r, fz_s, fz_r, fy_s, fy_r, wd_s, wd_r, a_s, a_r,
):
    ctx = lax.axis_index("ctx")
    x = lax.axis_index("mp")
    c = lax.rem(ctx, 2)
    z = lax.rem(ctx // 2, RING)
    y = ctx // (2 * RING)

    def place(yy, zz, cc):
        return (yy * RING + zz) * 2 + cc

    def plus(p, d):
        return lax.rem(p + d, RING)

    partner = {"ctx": place(y, z, 1 - c), "mp": x}

    def zpeer(p):
        return {"ctx": place(y, p, c), "mp": x}

    def ypeer(p):
        return {"ctx": place(p, z, c), "mp": x}

    def xpeer(p):
        return {"ctx": ctx, "mp": p}

    def rcopy(src, dst, s, r, dev):
        return pltpu.make_async_remote_copy(
            src_ref=src, dst_ref=dst, send_sem=s, recv_sem=r, device_id=dev, device_id_type=MESH
        )

    barrier = pltpu.get_barrier_semaphore()
    pl.semaphore_signal(barrier, inc=1, device_id=partner, device_id_type=MESH)
    for d in (1, 2, 3):
        for dev in (zpeer(plus(z, d)), ypeer(plus(y, d)), xpeer(plus(x, d))):
            pl.semaphore_signal(barrier, inc=1, device_id=dev, device_id_type=MESH)

    def rows(n, size=BLK):
        return pl.ds(pl.multiple_of(n * size, size), size)

    def kload(n):
        return pltpu.make_async_copy(k_hbm.at[rows(n)], kv.at[rows(n)], kvsem.at[0, n])

    def vload(n):
        return pltpu.make_async_copy(v_hbm.at[rows(n)], vv.at[rows(n)], kvsem.at[1, n])

    qload = pltpu.make_async_copy(q_hbm, qv, qsem)
    wload = pltpu.make_async_copy(w_hbm, wb.at[x], wsem)
    for n in range(NBLK):
        kload(n).start()
        vload(n).start()
        if n == 3:
            wload.start()
    qload.start()

    def leaf_body(n, carry):
        kload(n).wait()
        vload(n).wait()

        for h in range(HEADS):
            col = slice(h * DH, (h + 1) * DH)
            leaf[n, h] = dot_tl(kv[rows(n), col], vv[rows(n), col])
        return carry

    lax.fori_loop(0, NBLK, leaf_body, 0)
    for h in range(HEADS):
        total = leaf[0, h]
        for n in range(1, NBLK):
            total = total + leaf[n, h]
        tot[h] = total
        tsend[h] = total.astype(BF)

    pl.semaphore_wait(barrier, 10)
    tcopy = rcopy(tsend, trecv, t_s, t_r, partner)
    tcopy.start()

    def piece_a(quarter, p):
        return wb.at[quarter, rows(p, DH), pl.ds(pl.multiple_of(c * 1024, 1024), 512)]

    def piece_b(quarter, p):
        return wb.at[quarter, rows(p, DH), pl.ds(pl.multiple_of(c * 1024 + 512, 512), 512)]

    def wx_a(quarter, d):
        return rcopy(piece_a(quarter, z), piece_a(quarter, z), wx_s.at[d - 1, 0], wx_r.at[quarter, 0], xpeer(plus(x, d)))

    def wx_b(quarter, d):
        return rcopy(piece_b(quarter, y), piece_b(quarter, y), wx_s.at[d - 1, 1], wx_r.at[quarter, 1], xpeer(plus(x, d)))

    wload.wait()
    for d in (1, 3, 2):
        wx_a(x, d).start()
        wx_b(x, d).start()

    table = jnp.concatenate(
        [tab_ref[:, h, :] for h in range(HEADS)] + [jnp.zeros((16, DH - HEADS * LEVELS), F32)], axis=1
    )
    hi = table.astype(BF)
    rest = table - hi.astype(F32)
    mid = rest.astype(BF)
    low = (rest - mid.astype(F32)).astype(BF)
    table3 = jnp.concatenate([hi, mid, low], axis=0)
    plan = lax.broadcasted_iota(jnp.int32, (16, DH), 0)
    for i in range(TOK // DH):
        hot = (jnp.broadcast_to(idx_ref[i : i + 1, :], (16, DH)) == plan).astype(F32).astype(BF)
        wt[i * DH : (i + 1) * DH, :] = dot_tl(jnp.concatenate([hot, hot, hot], axis=0), table3)
    tt = lax.broadcasted_iota(jnp.int32, (HALF, HALF), 0)
    ss = lax.broadcasted_iota(jnp.int32, (HALF, HALF), 1)
    apart = jnp.bitwise_xor(tt, ss)
    level = jnp.zeros((HALF, HALF), jnp.int32)
    for bit in range(7):
        level = level + (apart >= (1 << bit)).astype(jnp.int32)
    for h in range(HEADS):
        pick[h] = jnp.where(ss <= tt, level + h * LEVELS, ZERO_LANE)

    zero = jnp.zeros((DH, DH), BF)

    for h in range(HEADS):
        l0, l2, l4, l6 = leaf[0, h], leaf[2, h], leaf[4, h], leaf[6, h]
        p0 = l0 + leaf[1, h]
        p4 = l4 + leaf[5, h]
        f0 = p0 + (l2 + leaf[3, h])
        near[h, 0] = zero
        for i, node in enumerate((l0, l2, l4, l6, p0, p4, f0)):
            near[h, 1 + i] = node.astype(BF)
    for p in range(2):
        far[p, 0 : REMOTE * DH, DH:] = jnp.zeros((REMOTE * DH, DH), BF)
        far[p, REMOTE * DH :, :DH] = jnp.zeros((REMOTE * DH, DH), BF)
    qload.wait()

    half0 = c * 2

    def far_at(pair, i, first, count):
        return far.at[pair, pl.ds((i * REMOTE + first) * DH, count * DH), pl.ds(i * DH, DH)]

    def zcopy(src, d, i):
        return rcopy(zr.at[src, i], zr.at[src, i], z_s.at[d - 1, i], z_r.at[src, i], zpeer(plus(z, d)))

    def ycopy(src, d, i):
        return rcopy(yr.at[src, i], yr.at[src, i], y_s.at[d - 1, i], y_r.at[src, i], ypeer(plus(y, d)))

    def lcopy(i):
        mine = far_at(c, i, 1, 4)
        return rcopy(mine, mine, l_s.at[i], l_r.at[i], partner)

    def choose(cond, value):
        return jnp.where(cond, value, jnp.zeros_like(value))

    def exchange_z():
        tcopy.wait_recv()
        for i in range(2):
            zr[z, i] = (tot[half0 + i] + trecv[half0 + i].astype(F32)).astype(BF)
            for d in (2, 1, 3):
                zcopy(z, d, i).start()
        for h in range(HEADS):
            far_at(h // 2, h % 2, 0, 1)[...] = choose(c == 1, trecv[h].astype(F32)).astype(BF)

    def exchange_y(i):
        for d in (1, 2, 3):
            zcopy(plus(z, d), d, i).wait_recv()
        parts = [zr[p, i].astype(F32) for p in range(RING)]
        pair = parts[0] + parts[1]
        yr[y, i] = (pair + (parts[2] + parts[3])).astype(BF)
        for d in (2, 1, 3):

            @pl.when(y + d < RING)
            def _():
                ycopy(y, d, i).start()

        lower = zr[jnp.maximum(z - 1, 0), i].astype(F32)
        far_at(c, i, 1, 1)[...] = choose(lax.rem(z, 2) == 1, lower).astype(BF)
        far_at(c, i, 2, 1)[...] = choose(z >= 2, pair).astype(BF)

    def exchange_end(i):
        for d in (1, 2, 3):

            @pl.when(y >= d)
            def _():
                ycopy(y - d, d, i).wait_recv()

        lower = yr[jnp.maximum(y - 1, 0), i].astype(F32)
        pair = yr[0, i].astype(F32) + yr[1, i].astype(F32)
        far_at(c, i, 3, 1)[...] = choose(lax.rem(y, 2) == 1, lower).astype(BF)
        far_at(c, i, 4, 1)[...] = choose(y >= 2, pair).astype(BF)
        lcopy(i).start()

    exchange_z()

    def attend(n):
        r = rows(n)
        w = wt[r, :]
        w16 = w.astype(BF)
        which = (
            jnp.where(lax.rem(n, 2) == 1, 1 + n // 2, 0),
            jnp.where(lax.rem(n // 2, 2) == 1, jnp.where(n >= 4, 6, 5), 0),
            jnp.where(n >= 4, 7, 0),
        )
        z_lo, z_hi = jnp.zeros((HALF, DH), BF), jnp.zeros((BLK, DH), BF)
        for p in range(2):
            low, high, near_q, values = [], [], [], []
            for h in (2 * p, 2 * p + 1):
                col = slice(h * DH, (h + 1) * DH)
                q, k, v = qv[r, col], kv[r, col], vv[r, col]
                at = pick[h]
                s_lo = dot_t(q[:HALF], k[:HALF])
                s_hi = dot_t(q[HALF:], k)
                low.append((s_lo * pick_lanes(w[:HALF], at)).astype(BF))
                high.append((s_hi[:, :HALF] * lanes(w16[HALF:], h * LEVELS + 8, HALF).astype(F32)).astype(BF))
                high.append((s_hi[:, HALF:] * pick_lanes(w[HALF:], at)).astype(BF))
                for j in range(LOCAL):
                    near_q.append(q * lanes(w16, h * LEVELS + 9 + j, BLK))
                for j in range(REMOTE):
                    ql_far[r, (h * REMOTE + j) * DH : (h * REMOTE + j + 1) * DH] = q * lanes(
                        w16, h * LEVELS + 12 + j, BLK
                    )
                values.append(v)
            va, vb = values
            nodes_a, nodes_b = ([near[h, t] for t in which] for h in (2 * p, 2 * p + 1))
            states = stacked(
                *[beside(t, zero) for t in nodes_a],
                *[beside(zero, t) for t in nodes_b],
            )
            pair = slice(2 * p * DH, 2 * (p + 1) * DH)
            acc[rows(2 * n, HALF), pair] = dot(
                beside(*low, *[t[:HALF] for t in near_q]),
                stacked(beside(va[:HALF], z_lo), beside(z_lo, vb[:HALF]), states),
            )
            acc[rows(2 * n + 1, HALF), pair] = dot(
                beside(*high, *[t[HALF:] for t in near_q]),
                stacked(beside(va, z_hi), beside(z_hi, vb), states),
            )

    order = (2, 1, 3)

    def offset(i):
        return jnp.where(i == 0, order[0], jnp.where(i == 1, order[1], order[2]))

    def attend_sent(i, carry):
        attend(2 * plus(x, offset(lax.rem(i, 3))) + i // 3)
        for at_i, hook in hooks:

            @pl.when(i == at_i)
            def _():
                hook()

        return carry

    def wz(quarter, src, d):
        return rcopy(piece_a(quarter, src), piece_a(quarter, src), wz_s.at[quarter, d - 1], wz_r.at[quarter, src], zpeer(plus(z, d)))

    def wy(quarter, src, d):
        return rcopy(piece_b(quarter, src), piece_b(quarter, src), wy_s.at[quarter, d - 1], wy_r.at[quarter, src], ypeer(plus(y, d)))

    sources = (3, 1, 2)

    def half_a(quarter, p, k):
        return wb.at[quarter, rows(2 * p + k, DH // 2), pl.ds(pl.multiple_of(c * 1024, 1024), 512)]

    def half_b(quarter, p, k):
        return wb.at[quarter, rows(2 * p + k, DH // 2), pl.ds(pl.multiple_of(c * 1024 + 512, 512), 512)]

    def fz(quarter, p, k, d):
        piece = half_a(quarter, p, k)
        return rcopy(piece, piece, fz_s.at[quarter, k], fz_r.at[quarter, k], zpeer(plus(z, d)))

    def fy(quarter, p, k, d):
        piece = half_b(quarter, p, k)
        return rcopy(piece, piece, fy_s.at[quarter, k], fy_r.at[quarter, k], ypeer(plus(y, d)))

    def send_wz(e):
        wx_a(plus(x, e), 1).wait_recv()
        for d in (1, 3):
            wz(plus(x, e), z, d).start()

    def send_wy(e):
        wx_b(plus(x, e), 1).wait_recv()
        for d in (1, 3):
            wy(plus(x, e), y, d).start()

    def forward_z(e):
        quarter = plus(x, e)
        wz(quarter, plus(z, 3), 1).wait_recv()
        fz(quarter, plus(z, 3), 0, 1).start()
        wz(quarter, plus(z, 1), 3).wait_recv()
        fz(quarter, plus(z, 1), 1, 3).start()

    def forward_y(e):
        quarter = plus(x, e)
        wy(quarter, plus(y, 3), 1).wait_recv()
        fy(quarter, plus(y, 3), 0, 1).start()
        wy(quarter, plus(y, 1), 3).wait_recv()
        fy(quarter, plus(y, 1), 1, 3).start()

    def wd(quarter, e, part):
        cols = pl.ds(pl.multiple_of(c * 1024 + part * 512, 512), 512)
        piece = wb.at[quarter, :, cols]
        return rcopy(piece, piece, wd_s.at[e - 1, part], wd_r.at[quarter, part], partner)

    def share_a(e):
        quarter = plus(x, e)
        for k in range(2):
            fz(quarter, plus(z, 2), k, 1 + 2 * k).wait_recv()
        wd(quarter, e, 0).start()

    def share_b(e):
        quarter = plus(x, e)
        for k in range(2):
            fy(quarter, plus(y, 2), k, 1 + 2 * k).wait_recv()
        wd(quarter, e, 1).start()

    hooks = (
        (4, lambda: exchange_y(0)),
        (5, lambda: exchange_y(1)),
    )
    lax.fori_loop(0, 6, attend_sent, 0)
    exchange_end(0)
    exchange_end(1)

    def acopy(src, slot, d):
        mine = lax.rem(slot + c, 2)
        block = 2 * plus(src, d)
        if slot < 2:
            cols = pl.ds(pl.multiple_of(mine * 2 * DH, 2 * DH), 2 * DH)
            here = nb.at[rows(block), cols]
            there = rb.at[src, pl.ds(0, BLK), cols]
        else:
            here = nb.at[rows(2 * block + slot, HALF)]
            there = rb.at[src, pl.ds(slot * HALF, HALF)]
        return rcopy(here, there, a_s.at[d - 1, slot], a_r.at[src, slot], xpeer(plus(src, d)))

    def finish(n, pair):
        r = rows(n)
        col = pl.ds(pl.multiple_of(pair * 2 * DH, 2 * DH), 2 * DH)
        wide = pl.ds(pl.multiple_of(pair * 2 * REMOTE * DH, 2 * REMOTE * DH), 2 * REMOTE * DH)
        o = acc[r, col] + dot(ql_far[r, wide], far[pair])
        done = []
        for t in (o[:, :DH], o[:, DH:]):
            ms = jnp.mean(t * t, axis=-1, keepdims=True)
            done.append((t * lax.rsqrt(ms + EPSILON)).astype(BF))
        nb[r, col] = beside(*done)

    def send_slots(i, slots):
        for m, d in enumerate(order):

            @pl.when(i == m)
            def _():
                for slot in slots:
                    acopy(x, slot, d).start()

    def early(slot):
        def body(i, carry):
            finish(2 * plus(x, offset(i)), lax.rem(slot + c, 2))
            send_slots(i, (slot,))
            return carry

        lax.fori_loop(0, 3, body, 0)

    def late(i, carry):
        n = 2 * plus(x, offset(i)) + 1
        finish(n, 0)
        finish(n, 1)
        send_slots(i, (2, 3))
        return carry

    early(0)
    send_wz(3)
    send_wz(1)
    send_wy(3)
    send_wy(1)
    for i in range(2):
        theirs = far_at(1 - c, i, 1, 4)
        rcopy(theirs, theirs, l_s.at[i], l_r.at[i], partner).wait_recv()
    early(1)
    send_wz(2)
    send_wy(2)
    lax.fori_loop(0, 3, late, 0)
    for e in sources:
        forward_z(e)
        forward_y(e)

    def keep(i, carry):
        attend(2 * x + i)
        finish(2 * x + i, 0)
        finish(2 * x + i, 1)
        return carry

    lax.fori_loop(0, 2, keep, 0)

    NC = 512

    def project_own(i, carry):
        cl = rows(i, NC)
        own[:, cl] = dot(nb[rows(x, OROWS), :], wb[x, :, cl])
        return carry

    def project(row, size):
        rws = pl.ds(row, size)

        def body(i, carry):
            cl = rows(i, NC)
            s = dot(rb[plus(x, sources[0]), rws, :], wb[plus(x, sources[0]), :, cl])
            for e in sources[1:]:
                s = s + dot(rb[plus(x, e), rws, :], wb[plus(x, e), :, cl])
            o_ref[rws, cl] = (s + own[rws, cl]).astype(BF)
            return carry

        lax.fori_loop(0, OUT // NC, body, 0)

    for e in sources:
        share_a(e)
        share_b(e)
    lax.fori_loop(0, OUT // NC, project_own, 0)
    for e in sources:
        for part in range(2):
            wd(plus(x, e), e, part).wait_recv()
    for slot in range(4):
        for e in sources:
            acopy(plus(x, e), slot, RING - e).wait_recv()
        if slot == 1:
            project(0, BLK)
        elif slot > 1:
            project(slot * HALF, HALF)

    tcopy.wait_send()
    for i in range(2):
        lcopy(i).wait_send()
    for d in (1, 2, 3):
        for i in range(2):
            zcopy(z, d, i).wait_send()

            @pl.when(y + d < RING)
            def _():
                ycopy(y, d, i).wait_send()

        wx_a(x, d).wait_send()
        wx_b(x, d).wait_send()
        quarter = plus(x, d)
        for k, dd in ((0, 1), (1, 3)):
            wz(quarter, z, dd).wait_send()
            wy(quarter, y, dd).wait_send()
            fz(quarter, plus(z, dd), k, dd).wait_send()
            fy(quarter, plus(y, dd), k, dd).wait_send()
            wd(quarter, d, k).wait_send()
        for slot in range(4):
            acopy(x, slot, d).wait_send()


def body(queries, key_vectors, value_vectors, level_index, level_table, out_weight):
    index = level_index.reshape(TOK // DH, DH)
    anyspec = pl.BlockSpec(memory_space=pl.ANY)
    vspec = pl.BlockSpec(memory_space=pltpu.VMEM)
    dma = pltpu.SemaphoreType.DMA
    scratch = [
        pltpu.VMEM((TOK, COLS), BF),
        pltpu.VMEM((TOK, COLS), BF),
        pltpu.VMEM((TOK, COLS), BF),
        pltpu.VMEM((RING, COLS, OUT), BF),
        pltpu.VMEM((TOK, DH), F32),
        pltpu.VMEM((HEADS, HALF, HALF), jnp.int32),
        pltpu.VMEM((NBLK, HEADS, DH, DH), F32),
        pltpu.VMEM((HEADS, 8, DH, DH), BF),
        pltpu.VMEM((HEADS, DH, DH), F32),
        pltpu.VMEM((HEADS, DH, DH), BF),
        pltpu.VMEM((HEADS, DH, DH), BF),
        pltpu.VMEM((RING, 2, DH, DH), BF),
        pltpu.VMEM((RING, 2, DH, DH), BF),
        pltpu.VMEM((2, 2 * REMOTE * DH, 2 * DH), BF),
        pltpu.VMEM((TOK, COLS), F32),
        pltpu.VMEM((TOK, HEADS * REMOTE * DH), BF),
        pltpu.VMEM((TOK, COLS), BF),
        pltpu.VMEM((RING, OROWS, COLS), BF),
        pltpu.VMEM((OROWS, OUT), F32),
        dma((2, NBLK)), dma, dma,
        dma, dma, dma((3, 2)), dma((RING, 2)), dma((3, 2)), dma((RING, 2)), dma((2,)), dma((2,)),
        dma((3, 2)), dma((RING, 2)), dma((RING, 3)), dma((RING, RING)), dma((RING, 3)), dma((RING, RING)),
        dma((RING, 2)), dma((RING, 2)), dma((RING, 2)), dma((RING, 2)),
        dma((3, 2)), dma((RING, 2)), dma((3, 4)), dma((RING, 4)),
    ]
    return pl.pallas_call(
        kernel,
        out_shape=pltpu.VMEM((OROWS, OUT), BF),
        in_specs=[vspec, vspec, anyspec, anyspec, anyspec, anyspec],
        out_specs=vspec,
        scratch_shapes=scratch,
        compiler_params=pltpu.CompilerParams(
            collective_id=0, has_side_effects=True, vmem_limit_bytes=56 * 1024 * 1024
        ),
    )(index, level_table, queries, key_vectors, value_vectors, out_weight)


def solution(mesh):
    placed = (
        P("ctx", "mp"),
        P("ctx", "mp"),
        P("ctx", "mp"),
        P("ctx"),
        P(None, "mp", None),
        P("mp", None),
    )
    return jax.shard_map(
        body, mesh=mesh, in_specs=placed, out_specs=P(("ctx", "mp"), None), check_vma=False
    )
```

```python
import functools

import jax
import jax.numpy as jnp
from jax import lax
from jax.experimental import pallas as pl
from jax.experimental.pallas import tpu as pltpu
from jax.sharding import PartitionSpec as P

EPSILON = 1e-06
BF = jnp.bfloat16
F32 = jnp.float32
MESH = pl.DeviceIdType.MESH

BLK = 256
HALF = 128
NBLK = 8
HEADS = 4
DH = 128
COLS = HEADS * DH
TOK = NBLK * BLK
RING = 4
OUT = 2048
OROWS = TOK // RING
LOCAL = 3
REMOTE = 5
LEVELS = 20
ZERO_LANE = 127


def dot(a, b):
    return jnp.dot(a, b, preferred_element_type=F32)


def dot_t(a, b):
    return lax.dot_general(a, b, (((1,), (1,)), ((), ())), preferred_element_type=F32)


def dot_tl(a, b):
    return lax.dot_general(a, b, (((0,), (0,)), ((), ())), preferred_element_type=F32)


GATHER = lax.GatherDimensionNumbers(
    offset_dims=(),
    collapsed_slice_dims=(1,),
    start_index_map=(1,),
    operand_batching_dims=(0,),
    start_indices_batching_dims=(0,),
)


def pick_lanes(w, at):
    return lax.gather(w, at[..., None], GATHER, (1, 1), mode=lax.GatherScatterMode.PROMISE_IN_BOUNDS)


def beside(*parts):
    return jnp.concatenate(parts, axis=1)


def stacked(*parts):
    return jnp.concatenate(parts, axis=0)


def lanes(w, lane, rows):
    return jnp.broadcast_to(w[:, lane : lane + 1], (rows, DH))


def kernel(
    idx_ref, tab_ref, q_hbm, k_hbm, v_hbm, w_hbm, o_ref,
    qv, kv, vv, wb, wt, pick, leaf, near, tot, tsend, trecv, zr, yr, far, acc, ql_far, nb, rb, own,
    kvsem, qsem, wsem,
    t_s, t_r, z_s, z_r, y_s, y_r, l_s, l_r,
    wx_s, wx_r, wz_s, wz_r, wy_s, wy_r, fz_s, fz_r, fy_s, fy_r, wd_s, wd_r, a_s, a_r,
):
    ctx = lax.axis_index("ctx")
    x = lax.axis_index("mp")
    c = lax.rem(ctx, 2)
    z = lax.rem(ctx // 2, RING)
    y = ctx // (2 * RING)

    def place(yy, zz, cc):
        return (yy * RING + zz) * 2 + cc

    def plus(p, d):
        return lax.rem(p + d, RING)

    partner = {"ctx": place(y, z, 1 - c), "mp": x}

    def zpeer(p):
        return {"ctx": place(y, p, c), "mp": x}

    def ypeer(p):
        return {"ctx": place(p, z, c), "mp": x}

    def xpeer(p):
        return {"ctx": ctx, "mp": p}

    def rcopy(src, dst, s, r, dev):
        return pltpu.make_async_remote_copy(
            src_ref=src, dst_ref=dst, send_sem=s, recv_sem=r, device_id=dev, device_id_type=MESH
        )

    barrier = pltpu.get_barrier_semaphore()
    pl.semaphore_signal(barrier, inc=1, device_id=partner, device_id_type=MESH)
    for d in (1, 2, 3):
        for dev in (zpeer(plus(z, d)), ypeer(plus(y, d)), xpeer(plus(x, d))):
            pl.semaphore_signal(barrier, inc=1, device_id=dev, device_id_type=MESH)

    def rows(n, size=BLK):
        return pl.ds(pl.multiple_of(n * size, size), size)

    def kload(n):
        return pltpu.make_async_copy(k_hbm.at[rows(n)], kv.at[rows(n)], kvsem.at[0, n])

    def vload(n):
        return pltpu.make_async_copy(v_hbm.at[rows(n)], vv.at[rows(n)], kvsem.at[1, n])

    qload = pltpu.make_async_copy(q_hbm, qv, qsem)
    wload = pltpu.make_async_copy(w_hbm, wb.at[x], wsem)
    for n in range(NBLK):
        kload(n).start()
        vload(n).start()
        if n == 3:
            wload.start()
    qload.start()

    def leaf_body(n, carry):
        kload(n).wait()
        vload(n).wait()

        for h in range(HEADS):
            col = slice(h * DH, (h + 1) * DH)
            leaf[n, h] = dot_tl(kv[rows(n), col], vv[rows(n), col])
        return carry

    lax.fori_loop(0, NBLK, leaf_body, 0)
    for h in range(HEADS):
        total = leaf[0, h]
        for n in range(1, NBLK):
            total = total + leaf[n, h]
        tot[h] = total
        tsend[h] = total.astype(BF)

    pl.semaphore_wait(barrier, 10)
    tcopy = rcopy(tsend, trecv, t_s, t_r, partner)
    tcopy.start()

    def piece_a(quarter, p):
        return wb.at[quarter, rows(p, DH), pl.ds(pl.multiple_of(c * 1024, 1024), 512)]

    def piece_b(quarter, p):
        return wb.at[quarter, rows(p, DH), pl.ds(pl.multiple_of(c * 1024 + 512, 512), 512)]

    def wx_a(quarter, d):
        return rcopy(piece_a(quarter, z), piece_a(quarter, z), wx_s.at[d - 1, 0], wx_r.at[quarter, 0], xpeer(plus(x, d)))

    def wx_b(quarter, d):
        return rcopy(piece_b(quarter, y), piece_b(quarter, y), wx_s.at[d - 1, 1], wx_r.at[quarter, 1], xpeer(plus(x, d)))

    wload.wait()
    for d in (1, 3, 2):
        wx_a(x, d).start()
        wx_b(x, d).start()

    table = jnp.concatenate(
        [tab_ref[:, h, :] for h in range(HEADS)] + [jnp.zeros((16, DH - HEADS * LEVELS), F32)], axis=1
    )
    hi = table.astype(BF)
    rest = table - hi.astype(F32)
    mid = rest.astype(BF)
    low = (rest - mid.astype(F32)).astype(BF)
    table3 = jnp.concatenate([hi, mid, low], axis=0)
    plan = lax.broadcasted_iota(jnp.int32, (16, DH), 0)
    for i in range(TOK // DH):
        hot = (jnp.broadcast_to(idx_ref[i : i + 1, :], (16, DH)) == plan).astype(F32).astype(BF)
        wt[i * DH : (i + 1) * DH, :] = dot_tl(jnp.concatenate([hot, hot, hot], axis=0), table3)
    tt = lax.broadcasted_iota(jnp.int32, (HALF, HALF), 0)
    ss = lax.broadcasted_iota(jnp.int32, (HALF, HALF), 1)
    apart = jnp.bitwise_xor(tt, ss)
    level = jnp.zeros((HALF, HALF), jnp.int32)
    for bit in range(7):
        level = level + (apart >= (1 << bit)).astype(jnp.int32)
    for h in range(HEADS):
        pick[h] = jnp.where(ss <= tt, level + h * LEVELS, ZERO_LANE)

    zero = jnp.zeros((DH, DH), BF)

    for h in range(HEADS):
        l0, l2, l4, l6 = leaf[0, h], leaf[2, h], leaf[4, h], leaf[6, h]
        p0 = l0 + leaf[1, h]
        p4 = l4 + leaf[5, h]
        f0 = p0 + (l2 + leaf[3, h])
        near[h, 0] = zero
        for i, node in enumerate((l0, l2, l4, l6, p0, p4, f0)):
            near[h, 1 + i] = node.astype(BF)
    for p in range(2):
        far[p, 0 : REMOTE * DH, DH:] = jnp.zeros((REMOTE * DH, DH), BF)
        far[p, REMOTE * DH :, :DH] = jnp.zeros((REMOTE * DH, DH), BF)
    qload.wait()

    half0 = c * 2

    def far_at(pair, i, first, count):
        return far.at[pair, pl.ds((i * REMOTE + first) * DH, count * DH), pl.ds(i * DH, DH)]

    def zcopy(src, d, i):
        return rcopy(zr.at[src, i], zr.at[src, i], z_s.at[d - 1, i], z_r.at[src, i], zpeer(plus(z, d)))

    def ycopy(src, d, i):
        return rcopy(yr.at[src, i], yr.at[src, i], y_s.at[d - 1, i], y_r.at[src, i], ypeer(plus(y, d)))

    def lcopy(i):
        mine = far_at(c, i, 1, 4)
        return rcopy(mine, mine, l_s.at[i], l_r.at[i], partner)

    def choose(cond, value):
        return jnp.where(cond, value, jnp.zeros_like(value))

    def exchange_z():
        tcopy.wait_recv()
        for i in range(2):
            zr[z, i] = (tot[half0 + i] + trecv[half0 + i].astype(F32)).astype(BF)
            for d in (2, 1, 3):
                zcopy(z, d, i).start()
        for h in range(HEADS):
            far_at(h // 2, h % 2, 0, 1)[...] = choose(c == 1, trecv[h].astype(F32)).astype(BF)

    def exchange_y(i):
        for d in (1, 2, 3):
            zcopy(plus(z, d), d, i).wait_recv()
        parts = [zr[p, i].astype(F32) for p in range(RING)]
        pair = parts[0] + parts[1]
        yr[y, i] = (pair + (parts[2] + parts[3])).astype(BF)
        for d in (2, 1, 3):

            @pl.when(y + d < RING)
            def _():
                ycopy(y, d, i).start()

        lower = zr[jnp.maximum(z - 1, 0), i].astype(F32)
        far_at(c, i, 1, 1)[...] = choose(lax.rem(z, 2) == 1, lower).astype(BF)
        far_at(c, i, 2, 1)[...] = choose(z >= 2, pair).astype(BF)

    def exchange_end(i):
        for d in (1, 2, 3):

            @pl.when(y >= d)
            def _():
                ycopy(y - d, d, i).wait_recv()

        lower = yr[jnp.maximum(y - 1, 0), i].astype(F32)
        pair = yr[0, i].astype(F32) + yr[1, i].astype(F32)
        far_at(c, i, 3, 1)[...] = choose(lax.rem(y, 2) == 1, lower).astype(BF)
        far_at(c, i, 4, 1)[...] = choose(y >= 2, pair).astype(BF)
        lcopy(i).start()

    exchange_z()

    def attend(n):
        r = rows(n)
        w = wt[r, :]
        w16 = w.astype(BF)
        which = (
            jnp.where(lax.rem(n, 2) == 1, 1 + n // 2, 0),
            jnp.where(lax.rem(n // 2, 2) == 1, jnp.where(n >= 4, 6, 5), 0),
            jnp.where(n >= 4, 7, 0),
        )
        z_lo, z_hi = jnp.zeros((HALF, DH), BF), jnp.zeros((BLK, DH), BF)
        for p in range(2):
            low, high, near_q, values = [], [], [], []
            for h in (2 * p, 2 * p + 1):
                col = slice(h * DH, (h + 1) * DH)
                q, k, v = qv[r, col], kv[r, col], vv[r, col]
                at = pick[h]
                s_lo = dot_t(q[:HALF], k[:HALF])
                s_hi = dot_t(q[HALF:], k)
                low.append((s_lo * pick_lanes(w[:HALF], at)).astype(BF))
                high.append((s_hi[:, :HALF] * lanes(w16[HALF:], h * LEVELS + 8, HALF).astype(F32)).astype(BF))
                high.append((s_hi[:, HALF:] * pick_lanes(w[HALF:], at)).astype(BF))
                for j in range(LOCAL):
                    near_q.append(q * lanes(w16, h * LEVELS + 9 + j, BLK))
                for j in range(REMOTE):
                    ql_far[r, (h * REMOTE + j) * DH : (h * REMOTE + j + 1) * DH] = q * lanes(
                        w16, h * LEVELS + 12 + j, BLK
                    )
                values.append(v)
            va, vb = values
            nodes_a, nodes_b = ([near[h, t] for t in which] for h in (2 * p, 2 * p + 1))
            states = stacked(
                *[beside(t, zero) for t in nodes_a],
                *[beside(zero, t) for t in nodes_b],
            )
            pair = slice(2 * p * DH, 2 * (p + 1) * DH)
            acc[rows(2 * n, HALF), pair] = dot(
                beside(*low, *[t[:HALF] for t in near_q]),
                stacked(beside(va[:HALF], z_lo), beside(z_lo, vb[:HALF]), states),
            )
            acc[rows(2 * n + 1, HALF), pair] = dot(
                beside(*high, *[t[HALF:] for t in near_q]),
                stacked(beside(va, z_hi), beside(z_hi, vb), states),
            )

    order = (2, 1, 3)

    def offset(i):
        return jnp.where(i == 0, order[0], jnp.where(i == 1, order[1], order[2]))

    def attend_sent(i, carry):
        attend(2 * plus(x, offset(lax.rem(i, 3))) + i // 3)
        for at_i, hook in hooks:

            @pl.when(i == at_i)
            def _():
                hook()

        return carry

    def wz(quarter, src, d):
        return rcopy(piece_a(quarter, src), piece_a(quarter, src), wz_s.at[quarter, d - 1], wz_r.at[quarter, src], zpeer(plus(z, d)))

    def wy(quarter, src, d):
        return rcopy(piece_b(quarter, src), piece_b(quarter, src), wy_s.at[quarter, d - 1], wy_r.at[quarter, src], ypeer(plus(y, d)))

    sources = (3, 1, 2)

    def half_a(quarter, p, k):
        return wb.at[quarter, rows(2 * p + k, DH // 2), pl.ds(pl.multiple_of(c * 1024, 1024), 512)]

    def half_b(quarter, p, k):
        return wb.at[quarter, rows(2 * p + k, DH // 2), pl.ds(pl.multiple_of(c * 1024 + 512, 512), 512)]

    def fz(quarter, p, k, d):
        piece = half_a(quarter, p, k)
        return rcopy(piece, piece, fz_s.at[quarter, k], fz_r.at[quarter, k], zpeer(plus(z, d)))

    def fy(quarter, p, k, d):
        piece = half_b(quarter, p, k)
        return rcopy(piece, piece, fy_s.at[quarter, k], fy_r.at[quarter, k], ypeer(plus(y, d)))

    def send_wz(e):
        wx_a(plus(x, e), 1).wait_recv()
        for d in (1, 3):
            wz(plus(x, e), z, d).start()

    def send_wy(e):
        wx_b(plus(x, e), 1).wait_recv()
        for d in (1, 3):
            wy(plus(x, e), y, d).start()

    def forward_z(e):
        quarter = plus(x, e)
        wz(quarter, plus(z, 3), 1).wait_recv()
        fz(quarter, plus(z, 3), 0, 1).start()
        wz(quarter, plus(z, 1), 3).wait_recv()
        fz(quarter, plus(z, 1), 1, 3).start()

    def forward_y(e):
        quarter = plus(x, e)
        wy(quarter, plus(y, 3), 1).wait_recv()
        fy(quarter, plus(y, 3), 0, 1).start()
        wy(quarter, plus(y, 1), 3).wait_recv()
        fy(quarter, plus(y, 1), 1, 3).start()

    def wd(quarter, e, part):
        cols = pl.ds(pl.multiple_of(c * 1024 + part * 512, 512), 512)
        piece = wb.at[quarter, :, cols]
        return rcopy(piece, piece, wd_s.at[e - 1, part], wd_r.at[quarter, part], partner)

    def share_a(e):
        quarter = plus(x, e)
        for k in range(2):
            fz(quarter, plus(z, 2), k, 1 + 2 * k).wait_recv()
        wd(quarter, e, 0).start()

    def share_b(e):
        quarter = plus(x, e)
        for k in range(2):
            fy(quarter, plus(y, 2), k, 1 + 2 * k).wait_recv()
        wd(quarter, e, 1).start()

    hooks = (
        (4, lambda: exchange_y(0)),
        (5, lambda: (exchange_y(1), send_wz(3), send_wz(1))),
    )
    lax.fori_loop(0, 6, attend_sent, 0)
    exchange_end(0)
    exchange_end(1)

    def acopy(src, slot, d):
        mine = lax.rem(slot + c, 2)
        block = 2 * plus(src, d)
        if slot < 2:
            cols = pl.ds(pl.multiple_of(mine * 2 * DH, 2 * DH), 2 * DH)
            here = nb.at[rows(block), cols]
            there = rb.at[src, pl.ds(0, BLK), cols]
        else:
            here = nb.at[rows(2 * block + slot, HALF)]
            there = rb.at[src, pl.ds(slot * HALF, HALF)]
        return rcopy(here, there, a_s.at[d - 1, slot], a_r.at[src, slot], xpeer(plus(src, d)))

    def finish(n, pair):
        r = rows(n)
        col = pl.ds(pl.multiple_of(pair * 2 * DH, 2 * DH), 2 * DH)
        wide = pl.ds(pl.multiple_of(pair * 2 * REMOTE * DH, 2 * REMOTE * DH), 2 * REMOTE * DH)
        o = acc[r, col] + dot(ql_far[r, wide], far[pair])
        done = []
        for t in (o[:, :DH], o[:, DH:]):
            ms = jnp.mean(t * t, axis=-1, keepdims=True)
            done.append((t * lax.rsqrt(ms + EPSILON)).astype(BF))
        nb[r, col] = beside(*done)

    def send_slots(i, slots):
        for m, d in enumerate(order):

            @pl.when(i == m)
            def _():
                for slot in slots:
                    acopy(x, slot, d).start()

    def early(slot):
        def body(i, carry):
            finish(2 * plus(x, offset(i)), lax.rem(slot + c, 2))
            send_slots(i, (slot,))
            return carry

        lax.fori_loop(0, 3, body, 0)

    def late(i, carry):
        n = 2 * plus(x, offset(i)) + 1
        finish(n, 0)
        finish(n, 1)
        send_slots(i, (2, 3))
        return carry

    send_wy(3)
    send_wy(1)
    early(0)
    for i in range(2):
        theirs = far_at(1 - c, i, 1, 4)
        rcopy(theirs, theirs, l_s.at[i], l_r.at[i], partner).wait_recv()
    early(1)
    send_wz(2)
    send_wy(2)
    lax.fori_loop(0, 3, late, 0)
    forward_z(3)
    forward_y(3)
    forward_z(1)

    def keep(i, carry):
        attend(2 * x + i)
        finish(2 * x + i, 0)
        finish(2 * x + i, 1)

        @pl.when(i == 0)
        def _():
            forward_y(1)
            forward_z(2)
            share_a(3)
            share_b(3)

        return carry

    lax.fori_loop(0, 2, keep, 0)

    NC = 512

    def project_own(i, carry):
        cl = rows(i, NC)
        own[:, cl] = dot(nb[rows(x, OROWS), :], wb[x, :, cl])
        return carry

    def project(row, size):
        rws = pl.ds(row, size)

        def body(i, carry):
            cl = rows(i, NC)
            s = dot(rb[plus(x, sources[0]), rws, :], wb[plus(x, sources[0]), :, cl])
            for e in sources[1:]:
                s = s + dot(rb[plus(x, e), rws, :], wb[plus(x, e), :, cl])
            o_ref[rws, cl] = (s + own[rws, cl]).astype(BF)
            return carry

        lax.fori_loop(0, OUT // NC, body, 0)

    def share_done(e):
        for part in range(2):
            wd(plus(x, e), e, part).wait_recv()

    def arrived(slot, es):
        for e in es:
            acopy(plus(x, e), slot, RING - e).wait_recv()

    forward_y(2)
    share_a(1)
    share_b(1)
    lax.fori_loop(0, OUT // NC, project_own, 0)
    share_a(2)
    share_b(2)
    share_done(3)
    share_done(1)
    share_done(2)
    arrived(0, sources)
    arrived(1, sources)
    project(0, BLK)
    for slot in (2, 3):
        arrived(slot, sources)
        project(slot * HALF, HALF)

    tcopy.wait_send()
    for i in range(2):
        lcopy(i).wait_send()
    for d in (1, 2, 3):
        for i in range(2):
            zcopy(z, d, i).wait_send()

            @pl.when(y + d < RING)
            def _():
                ycopy(y, d, i).wait_send()

        wx_a(x, d).wait_send()
        wx_b(x, d).wait_send()
        quarter = plus(x, d)
        for k, dd in ((0, 1), (1, 3)):
            wz(quarter, z, dd).wait_send()
            wy(quarter, y, dd).wait_send()
            fz(quarter, plus(z, dd), k, dd).wait_send()
            fy(quarter, plus(y, dd), k, dd).wait_send()
            wd(quarter, d, k).wait_send()
        for slot in range(4):
            acopy(x, slot, d).wait_send()


def body(queries, key_vectors, value_vectors, level_index, level_table, out_weight):
    index = level_index.reshape(TOK // DH, DH)
    anyspec = pl.BlockSpec(memory_space=pl.ANY)
    vspec = pl.BlockSpec(memory_space=pltpu.VMEM)
    dma = pltpu.SemaphoreType.DMA
    scratch = [
        pltpu.VMEM((TOK, COLS), BF),
        pltpu.VMEM((TOK, COLS), BF),
        pltpu.VMEM((TOK, COLS), BF),
        pltpu.VMEM((RING, COLS, OUT), BF),
        pltpu.VMEM((TOK, DH), F32),
        pltpu.VMEM((HEADS, HALF, HALF), jnp.int32),
        pltpu.VMEM((NBLK, HEADS, DH, DH), F32),
        pltpu.VMEM((HEADS, 8, DH, DH), BF),
        pltpu.VMEM((HEADS, DH, DH), F32),
        pltpu.VMEM((HEADS, DH, DH), BF),
        pltpu.VMEM((HEADS, DH, DH), BF),
        pltpu.VMEM((RING, 2, DH, DH), BF),
        pltpu.VMEM((RING, 2, DH, DH), BF),
        pltpu.VMEM((2, 2 * REMOTE * DH, 2 * DH), BF),
        pltpu.VMEM((TOK, COLS), F32),
        pltpu.VMEM((TOK, HEADS * REMOTE * DH), BF),
        pltpu.VMEM((TOK, COLS), BF),
        pltpu.VMEM((RING, OROWS, COLS), BF),
        pltpu.VMEM((OROWS, OUT), F32),
        dma((2, NBLK)), dma, dma,
        dma, dma, dma((3, 2)), dma((RING, 2)), dma((3, 2)), dma((RING, 2)), dma((2,)), dma((2,)),
        dma((3, 2)), dma((RING, 2)), dma((RING, 3)), dma((RING, RING)), dma((RING, 3)), dma((RING, RING)),
        dma((RING, 2)), dma((RING, 2)), dma((RING, 2)), dma((RING, 2)),
        dma((3, 2)), dma((RING, 2)), dma((3, 4)), dma((RING, 4)),
    ]
    return pl.pallas_call(
        kernel,
        out_shape=pltpu.VMEM((OROWS, OUT), BF),
        in_specs=[vspec, vspec, anyspec, anyspec, anyspec, anyspec],
        out_specs=vspec,
        scratch_shapes=scratch,
        compiler_params=pltpu.CompilerParams(
            collective_id=0, has_side_effects=True, vmem_limit_bytes=56 * 1024 * 1024
        ),
    )(index, level_table, queries, key_vectors, value_vectors, out_weight)


def solution(mesh):
    placed = (
        P("ctx", "mp"),
        P("ctx", "mp"),
        P("ctx", "mp"),
        P("ctx"),
        P(None, "mp", None),
        P("mp", None),
    )
    return jax.shard_map(
        body, mesh=mesh, in_specs=placed, out_specs=P(("ctx", "mp"), None), check_vma=False
    )
```

```python
import functools

import jax
import jax.numpy as jnp
from jax import lax
from jax.experimental import pallas as pl
from jax.experimental.pallas import tpu as pltpu
from jax.sharding import PartitionSpec as P

EPSILON = 1e-06
BF = jnp.bfloat16
F32 = jnp.float32
MESH = pl.DeviceIdType.MESH

BLK = 256
HALF = 128
NBLK = 8
HEADS = 4
DH = 128
COLS = HEADS * DH
TOK = NBLK * BLK
RING = 4
OUT = 2048
OROWS = TOK // RING
LOCAL = 3
REMOTE = 5
LEVELS = 20
ZERO_LANE = 127


def dot(a, b):
    return jnp.dot(a, b, preferred_element_type=F32)


def dot_t(a, b):
    return lax.dot_general(a, b, (((1,), (1,)), ((), ())), preferred_element_type=F32)


def dot_tl(a, b):
    return lax.dot_general(a, b, (((0,), (0,)), ((), ())), preferred_element_type=F32)


GATHER = lax.GatherDimensionNumbers(
    offset_dims=(),
    collapsed_slice_dims=(1,),
    start_index_map=(1,),
    operand_batching_dims=(0,),
    start_indices_batching_dims=(0,),
)


def pick_lanes(w, at):
    return lax.gather(w, at[..., None], GATHER, (1, 1), mode=lax.GatherScatterMode.PROMISE_IN_BOUNDS)


def beside(*parts):
    return jnp.concatenate(parts, axis=1)


def stacked(*parts):
    return jnp.concatenate(parts, axis=0)


def lanes(w, lane, rows):
    return jnp.broadcast_to(w[:, lane : lane + 1], (rows, DH))


def kernel(
    idx_ref, tab_ref, q_hbm, k_hbm, v_hbm, w_hbm, o_ref,
    qv, kv, vv, wb, wt, pick, leaf, near, tot, tsend, trecv, zr, yr, far, acc, ql_far, nb, rb, own,
    kvsem, qsem, wsem,
    t_s, t_r, z_s, z_r, y_s, y_r, l_s, l_r,
    wx_s, wx_r, wz_s, wz_r, wy_s, wy_r, fz_s, fz_r, fy_s, fy_r, wd_s, wd_r, a_s, a_r,
):
    ctx = lax.axis_index("ctx")
    x = lax.axis_index("mp")
    c = lax.rem(ctx, 2)
    z = lax.rem(ctx // 2, RING)
    y = ctx // (2 * RING)

    def place(yy, zz, cc):
        return (yy * RING + zz) * 2 + cc

    def plus(p, d):
        return lax.rem(p + d, RING)

    partner = {"ctx": place(y, z, 1 - c), "mp": x}

    def zpeer(p):
        return {"ctx": place(y, p, c), "mp": x}

    def ypeer(p):
        return {"ctx": place(p, z, c), "mp": x}

    def xpeer(p):
        return {"ctx": ctx, "mp": p}

    def rcopy(src, dst, s, r, dev):
        return pltpu.make_async_remote_copy(
            src_ref=src, dst_ref=dst, send_sem=s, recv_sem=r, device_id=dev, device_id_type=MESH
        )

    barrier = pltpu.get_barrier_semaphore()
    pl.semaphore_signal(barrier, inc=1, device_id=partner, device_id_type=MESH)
    for d in (1, 2, 3):
        for dev in (zpeer(plus(z, d)), ypeer(plus(y, d)), xpeer(plus(x, d))):
            pl.semaphore_signal(barrier, inc=1, device_id=dev, device_id_type=MESH)

    def rows(n, size=BLK):
        return pl.ds(pl.multiple_of(n * size, size), size)

    def kload(n):
        return pltpu.make_async_copy(k_hbm.at[rows(n)], kv.at[rows(n)], kvsem.at[0, n])

    def vload(n):
        return pltpu.make_async_copy(v_hbm.at[rows(n)], vv.at[rows(n)], kvsem.at[1, n])

    qload = pltpu.make_async_copy(q_hbm, qv, qsem)
    wload = pltpu.make_async_copy(w_hbm, wb.at[x], wsem)
    for n in range(NBLK):
        kload(n).start()
        vload(n).start()
        if n == 3:
            wload.start()
    qload.start()

    def leaf_body(n, carry):
        kload(n).wait()
        vload(n).wait()

        for h in range(HEADS):
            col = slice(h * DH, (h + 1) * DH)
            leaf[n, h] = dot_tl(kv[rows(n), col], vv[rows(n), col])
        return carry

    lax.fori_loop(0, NBLK, leaf_body, 0)
    for h in range(HEADS):
        total = leaf[0, h]
        for n in range(1, NBLK):
            total = total + leaf[n, h]
        tot[h] = total
        tsend[h] = total.astype(BF)

    pl.semaphore_wait(barrier, 10)
    tcopy = rcopy(tsend, trecv, t_s, t_r, partner)
    tcopy.start()

    def piece_a(quarter, p):
        return wb.at[quarter, rows(p, DH), pl.ds(pl.multiple_of(c * 1024, 1024), 512)]

    def piece_b(quarter, p):
        return wb.at[quarter, rows(p, DH), pl.ds(pl.multiple_of(c * 1024 + 512, 512), 512)]

    def wx_a(quarter, d):
        return rcopy(piece_a(quarter, z), piece_a(quarter, z), wx_s.at[d - 1, 0], wx_r.at[quarter, 0], xpeer(plus(x, d)))

    def wx_b(quarter, d):
        return rcopy(piece_b(quarter, y), piece_b(quarter, y), wx_s.at[d - 1, 1], wx_r.at[quarter, 1], xpeer(plus(x, d)))

    wload.wait()
    for d in (1, 3, 2):
        wx_a(x, d).start()
        wx_b(x, d).start()

    table = jnp.concatenate(
        [tab_ref[:, h, :] for h in range(HEADS)] + [jnp.zeros((16, DH - HEADS * LEVELS), F32)], axis=1
    )
    hi = table.astype(BF)
    rest = table - hi.astype(F32)
    mid = rest.astype(BF)
    low = (rest - mid.astype(F32)).astype(BF)
    table3 = jnp.concatenate([hi, mid, low], axis=0)
    plan = lax.broadcasted_iota(jnp.int32, (16, DH), 0)
    for i in range(TOK // DH):
        hot = (jnp.broadcast_to(idx_ref[i : i + 1, :], (16, DH)) == plan).astype(F32).astype(BF)
        wt[i * DH : (i + 1) * DH, :] = dot_tl(jnp.concatenate([hot, hot, hot], axis=0), table3)
    tt = lax.broadcasted_iota(jnp.int32, (HALF, HALF), 0)
    ss = lax.broadcasted_iota(jnp.int32, (HALF, HALF), 1)
    apart = jnp.bitwise_xor(tt, ss)
    level = jnp.zeros((HALF, HALF), jnp.int32)
    for bit in range(7):
        level = level + (apart >= (1 << bit)).astype(jnp.int32)
    for h in range(HEADS):
        pick[h] = jnp.where(ss <= tt, level + h * LEVELS, ZERO_LANE)

    zero = jnp.zeros((DH, DH), BF)

    for h in range(HEADS):
        l0, l2, l4, l6 = leaf[0, h], leaf[2, h], leaf[4, h], leaf[6, h]
        p0 = l0 + leaf[1, h]
        p4 = l4 + leaf[5, h]
        f0 = p0 + (l2 + leaf[3, h])
        near[h, 0] = zero
        for i, node in enumerate((l0, l2, l4, l6, p0, p4, f0)):
            near[h, 1 + i] = node.astype(BF)
    for p in range(2):
        far[p, 0 : REMOTE * DH, DH:] = jnp.zeros((REMOTE * DH, DH), BF)
        far[p, REMOTE * DH :, :DH] = jnp.zeros((REMOTE * DH, DH), BF)
    qload.wait()

    half0 = c * 2

    def far_at(pair, i, first, count):
        return far.at[pair, pl.ds((i * REMOTE + first) * DH, count * DH), pl.ds(i * DH, DH)]

    def zcopy(src, d, i):
        return rcopy(zr.at[src, i], zr.at[src, i], z_s.at[d - 1, i], z_r.at[src, i], zpeer(plus(z, d)))

    def ycopy(src, d, i):
        return rcopy(yr.at[src, i], yr.at[src, i], y_s.at[d - 1, i], y_r.at[src, i], ypeer(plus(y, d)))

    def lcopy(i):
        mine = far_at(c, i, 1, 4)
        return rcopy(mine, mine, l_s.at[i], l_r.at[i], partner)

    def choose(cond, value):
        return jnp.where(cond, value, jnp.zeros_like(value))

    def exchange_z():
        tcopy.wait_recv()
        for i in range(2):
            zr[z, i] = (tot[half0 + i] + trecv[half0 + i].astype(F32)).astype(BF)
            for d in (2, 1, 3):
                zcopy(z, d, i).start()
        for h in range(HEADS):
            far_at(h // 2, h % 2, 0, 1)[...] = choose(c == 1, trecv[h].astype(F32)).astype(BF)

    def exchange_y(i):
        for d in (1, 2, 3):
            zcopy(plus(z, d), d, i).wait_recv()
        parts = [zr[p, i].astype(F32) for p in range(RING)]
        pair = parts[0] + parts[1]
        yr[y, i] = (pair + (parts[2] + parts[3])).astype(BF)
        for d in (2, 1, 3):

            @pl.when(y + d < RING)
            def _():
                ycopy(y, d, i).start()

        lower = zr[jnp.maximum(z - 1, 0), i].astype(F32)
        far_at(c, i, 1, 1)[...] = choose(lax.rem(z, 2) == 1, lower).astype(BF)
        far_at(c, i, 2, 1)[...] = choose(z >= 2, pair).astype(BF)

    def exchange_end(i):
        for d in (1, 2, 3):

            @pl.when(y >= d)
            def _():
                ycopy(y - d, d, i).wait_recv()

        lower = yr[jnp.maximum(y - 1, 0), i].astype(F32)
        pair = yr[0, i].astype(F32) + yr[1, i].astype(F32)
        far_at(c, i, 3, 1)[...] = choose(lax.rem(y, 2) == 1, lower).astype(BF)
        far_at(c, i, 4, 1)[...] = choose(y >= 2, pair).astype(BF)
        lcopy(i).start()

    exchange_z()

    def attend(n):
        r = rows(n)
        w = wt[r, :]
        w16 = w.astype(BF)
        which = (
            jnp.where(lax.rem(n, 2) == 1, 1 + n // 2, 0),
            jnp.where(lax.rem(n // 2, 2) == 1, jnp.where(n >= 4, 6, 5), 0),
            jnp.where(n >= 4, 7, 0),
        )
        z_lo, z_hi = jnp.zeros((HALF, DH), BF), jnp.zeros((BLK, DH), BF)
        for p in range(2):
            low, high, near_q, values = [], [], [], []
            for h in (2 * p, 2 * p + 1):
                col = slice(h * DH, (h + 1) * DH)
                q, k, v = qv[r, col], kv[r, col], vv[r, col]
                at = pick[h]
                s_lo = dot_t(q[:HALF], k[:HALF])
                s_hi = dot_t(q[HALF:], k)
                low.append((s_lo * pick_lanes(w[:HALF], at)).astype(BF))
                high.append((s_hi[:, :HALF] * lanes(w16[HALF:], h * LEVELS + 8, HALF).astype(F32)).astype(BF))
                high.append((s_hi[:, HALF:] * pick_lanes(w[HALF:], at)).astype(BF))
                for j in range(LOCAL):
                    near_q.append(q * lanes(w16, h * LEVELS + 9 + j, BLK))
                for j in range(REMOTE):
                    ql_far[r, (h * REMOTE + j) * DH : (h * REMOTE + j + 1) * DH] = q * lanes(
                        w16, h * LEVELS + 12 + j, BLK
                    )
                values.append(v)
            va, vb = values
            nodes_a, nodes_b = ([near[h, t] for t in which] for h in (2 * p, 2 * p + 1))
            states = stacked(
                *[beside(t, zero) for t in nodes_a],
                *[beside(zero, t) for t in nodes_b],
            )
            pair = slice(2 * p * DH, 2 * (p + 1) * DH)
            acc[rows(2 * n, HALF), pair] = dot(
                beside(*low, *[t[:HALF] for t in near_q]),
                stacked(beside(va[:HALF], z_lo), beside(z_lo, vb[:HALF]), states),
            )
            acc[rows(2 * n + 1, HALF), pair] = dot(
                beside(*high, *[t[HALF:] for t in near_q]),
                stacked(beside(va, z_hi), beside(z_hi, vb), states),
            )

    order = (2, 1, 3)

    def offset(i):
        return jnp.where(i == 0, order[0], jnp.where(i == 1, order[1], order[2]))

    def attend_sent(i, carry):
        attend(2 * plus(x, offset(lax.rem(i, 3))) + i // 3)
        for at_i, hook in hooks:

            @pl.when(i == at_i)
            def _():
                hook()

        return carry

    def wz(quarter, src, d):
        return rcopy(piece_a(quarter, src), piece_a(quarter, src), wz_s.at[quarter, d - 1], wz_r.at[quarter, src], zpeer(plus(z, d)))

    def wy(quarter, src, d):
        return rcopy(piece_b(quarter, src), piece_b(quarter, src), wy_s.at[quarter, d - 1], wy_r.at[quarter, src], ypeer(plus(y, d)))

    sources = (3, 1, 2)

    def half_a(quarter, p, k):
        return wb.at[quarter, rows(2 * p + k, DH // 2), pl.ds(pl.multiple_of(c * 1024, 1024), 512)]

    def half_b(quarter, p, k):
        return wb.at[quarter, rows(2 * p + k, DH // 2), pl.ds(pl.multiple_of(c * 1024 + 512, 512), 512)]

    def fz(quarter, p, k, d):
        piece = half_a(quarter, p, k)
        return rcopy(piece, piece, fz_s.at[quarter, k], fz_r.at[quarter, k], zpeer(plus(z, d)))

    def fy(quarter, p, k, d):
        piece = half_b(quarter, p, k)
        return rcopy(piece, piece, fy_s.at[quarter, k], fy_r.at[quarter, k], ypeer(plus(y, d)))

    def send_wz(e):
        wx_a(plus(x, e), 1).wait_recv()
        for d in (1, 3):
            wz(plus(x, e), z, d).start()

    def send_wy(e):
        wx_b(plus(x, e), 1).wait_recv()
        for d in (1, 3):
            wy(plus(x, e), y, d).start()

    def forward_z(e):
        quarter = plus(x, e)
        wz(quarter, plus(z, 3), 1).wait_recv()
        fz(quarter, plus(z, 3), 0, 1).start()
        wz(quarter, plus(z, 1), 3).wait_recv()
        fz(quarter, plus(z, 1), 1, 3).start()

    def forward_y(e):
        quarter = plus(x, e)
        wy(quarter, plus(y, 3), 1).wait_recv()
        fy(quarter, plus(y, 3), 0, 1).start()
        wy(quarter, plus(y, 1), 3).wait_recv()
        fy(quarter, plus(y, 1), 1, 3).start()

    def wd(quarter, e, part):
        cols = pl.ds(pl.multiple_of(c * 1024 + part * 512, 512), 512)
        piece = wb.at[quarter, :, cols]
        return rcopy(piece, piece, wd_s.at[e - 1, part], wd_r.at[quarter, part], partner)

    def share_a(e):
        quarter = plus(x, e)
        for k in range(2):
            fz(quarter, plus(z, 2), k, 1 + 2 * k).wait_recv()
        wd(quarter, e, 0).start()

    def share_b(e):
        quarter = plus(x, e)
        for k in range(2):
            fy(quarter, plus(y, 2), k, 1 + 2 * k).wait_recv()
        wd(quarter, e, 1).start()

    hooks = (
        (3, lambda: exchange_y(0)),
        (4, lambda: exchange_y(1)), (5, lambda: (send_wz(3), send_wz(1))),
    )
    lax.fori_loop(0, 6, attend_sent, 0)
    exchange_end(0)
    exchange_end(1)

    def acopy(src, slot, d):
        mine = lax.rem(slot + c, 2)
        block = 2 * plus(src, d)
        if slot < 2:
            cols = pl.ds(pl.multiple_of(mine * 2 * DH, 2 * DH), 2 * DH)
            here = nb.at[rows(block), cols]
            there = rb.at[src, pl.ds(0, BLK), cols]
        else:
            here = nb.at[rows(2 * block + slot, HALF)]
            there = rb.at[src, pl.ds(slot * HALF, HALF)]
        return rcopy(here, there, a_s.at[d - 1, slot], a_r.at[src, slot], xpeer(plus(src, d)))

    def finish(n, pair):
        r = rows(n)
        col = pl.ds(pl.multiple_of(pair * 2 * DH, 2 * DH), 2 * DH)
        wide = pl.ds(pl.multiple_of(pair * 2 * REMOTE * DH, 2 * REMOTE * DH), 2 * REMOTE * DH)
        o = acc[r, col] + dot(ql_far[r, wide], far[pair])
        done = []
        for t in (o[:, :DH], o[:, DH:]):
            ms = jnp.mean(t * t, axis=-1, keepdims=True)
            done.append((t * lax.rsqrt(ms + EPSILON)).astype(BF))
        nb[r, col] = beside(*done)

    def send_slots(i, slots):
        for m, d in enumerate(order):

            @pl.when(i == m)
            def _():
                for slot in slots:
                    acopy(x, slot, d).start()

    def early(slot):
        def body(i, carry):
            finish(2 * plus(x, offset(i)), lax.rem(slot + c, 2))
            send_slots(i, (slot,))
            return carry

        lax.fori_loop(0, 3, body, 0)

    def late(i, carry):
        n = 2 * plus(x, offset(i)) + 1
        finish(n, 0)
        finish(n, 1)
        send_slots(i, (2, 3))
        return carry

    send_wy(3)
    send_wy(1)
    early(0)
    for i in range(2):
        theirs = far_at(1 - c, i, 1, 4)
        rcopy(theirs, theirs, l_s.at[i], l_r.at[i], partner).wait_recv()
    early(1)
    send_wz(2)
    send_wy(2)
    lax.fori_loop(0, 3, late, 0)
    forward_z(3)
    forward_y(3)
    forward_z(1)

    def keep(i, carry):
        attend(2 * x + i)
        finish(2 * x + i, 0)
        finish(2 * x + i, 1)

        @pl.when(i == 0)
        def _():
            forward_y(1)
            forward_z(2)
            share_a(3)
            share_b(3)

        return carry

    lax.fori_loop(0, 2, keep, 0)

    NC = 512

    def project_own(i, carry):
        cl = rows(i, NC)
        own[:, cl] = dot(nb[rows(x, OROWS), :], wb[x, :, cl])
        return carry

    def project(row, size, es=sources, last=True):
        rws = pl.ds(row, size)

        def body(i, carry):
            cl = rows(i, NC)
            s = dot(rb[plus(x, es[0]), rws, :], wb[plus(x, es[0]), :, cl])
            for e in es[1:]:
                s = s + dot(rb[plus(x, e), rws, :], wb[plus(x, e), :, cl])
            s = s + own[rws, cl]
            if last:
                o_ref[rws, cl] = s.astype(BF)
            else:
                own[rws, cl] = s
            return carry

        lax.fori_loop(0, OUT // NC, body, 0)

    def share_done(e):
        for part in range(2):
            wd(plus(x, e), e, part).wait_recv()

    def arrived(slot, es):
        for e in es:
            acopy(plus(x, e), slot, RING - e).wait_recv()

    forward_y(2)
    share_a(1)
    share_b(1)
    lax.fori_loop(0, OUT // NC, project_own, 0)
    share_a(2)
    share_b(2)
    share_done(3)
    share_done(1)
    share_done(2)
    arrived(0, sources)
    arrived(1, sources)
    project(0, BLK)
    arrived(2, sources)
    project(2 * HALF, HALF)
    arrived(3, (2,))
    project(3 * HALF, HALF, (2,), False)
    arrived(3, (3, 1))
    project(3 * HALF, HALF, (3, 1))

    tcopy.wait_send()
    for i in range(2):
        lcopy(i).wait_send()
    for d in (1, 2, 3):
        for i in range(2):
            zcopy(z, d, i).wait_send()

            @pl.when(y + d < RING)
            def _():
                ycopy(y, d, i).wait_send()

        wx_a(x, d).wait_send()
        wx_b(x, d).wait_send()
        quarter = plus(x, d)
        for k, dd in ((0, 1), (1, 3)):
            wz(quarter, z, dd).wait_send()
            wy(quarter, y, dd).wait_send()
            fz(quarter, plus(z, dd), k, dd).wait_send()
            fy(quarter, plus(y, dd), k, dd).wait_send()
            wd(quarter, d, k).wait_send()
        for slot in range(4):
            acopy(x, slot, d).wait_send()


def body(queries, key_vectors, value_vectors, level_index, level_table, out_weight):
    index = level_index.reshape(TOK // DH, DH)
    anyspec = pl.BlockSpec(memory_space=pl.ANY)
    vspec = pl.BlockSpec(memory_space=pltpu.VMEM)
    dma = pltpu.SemaphoreType.DMA
    scratch = [
        pltpu.VMEM((TOK, COLS), BF),
        pltpu.VMEM((TOK, COLS), BF),
        pltpu.VMEM((TOK, COLS), BF),
        pltpu.VMEM((RING, COLS, OUT), BF),
        pltpu.VMEM((TOK, DH), F32),
        pltpu.VMEM((HEADS, HALF, HALF), jnp.int32),
        pltpu.VMEM((NBLK, HEADS, DH, DH), F32),
        pltpu.VMEM((HEADS, 8, DH, DH), BF),
        pltpu.VMEM((HEADS, DH, DH), F32),
        pltpu.VMEM((HEADS, DH, DH), BF),
        pltpu.VMEM((HEADS, DH, DH), BF),
        pltpu.VMEM((RING, 2, DH, DH), BF),
        pltpu.VMEM((RING, 2, DH, DH), BF),
        pltpu.VMEM((2, 2 * REMOTE * DH, 2 * DH), BF),
        pltpu.VMEM((TOK, COLS), F32),
        pltpu.VMEM((TOK, HEADS * REMOTE * DH), BF),
        pltpu.VMEM((TOK, COLS), BF),
        pltpu.VMEM((RING, OROWS, COLS), BF),
        pltpu.VMEM((OROWS, OUT), F32),
        dma((2, NBLK)), dma, dma,
        dma, dma, dma((3, 2)), dma((RING, 2)), dma((3, 2)), dma((RING, 2)), dma((2,)), dma((2,)),
        dma((3, 2)), dma((RING, 2)), dma((RING, 3)), dma((RING, RING)), dma((RING, 3)), dma((RING, RING)),
        dma((RING, 2)), dma((RING, 2)), dma((RING, 2)), dma((RING, 2)),
        dma((3, 2)), dma((RING, 2)), dma((3, 4)), dma((RING, 4)),
    ]
    return pl.pallas_call(
        kernel,
        out_shape=pltpu.VMEM((OROWS, OUT), BF),
        in_specs=[vspec, vspec, anyspec, anyspec, anyspec, anyspec],
        out_specs=vspec,
        scratch_shapes=scratch,
        compiler_params=pltpu.CompilerParams(
            collective_id=0, has_side_effects=True, vmem_limit_bytes=56 * 1024 * 1024
        ),
    )(index, level_table, queries, key_vectors, value_vectors, out_weight)


def solution(mesh):
    placed = (
        P("ctx", "mp"),
        P("ctx", "mp"),
        P("ctx", "mp"),
        P("ctx"),
        P(None, "mp", None),
        P("mp", None),
    )
    return jax.shard_map(
        body, mesh=mesh, in_specs=placed, out_specs=P(("ctx", "mp"), None), check_vma=False
    )
```

```python
import functools

import jax
import jax.numpy as jnp
from jax import lax
from jax.experimental import pallas as pl
from jax.experimental.pallas import tpu as pltpu
from jax.sharding import PartitionSpec as P

EPSILON = 1e-06
BF = jnp.bfloat16
F32 = jnp.float32
MESH = pl.DeviceIdType.MESH

BLK = 256
HALF = 128
NBLK = 8
HEADS = 4
DH = 128
COLS = HEADS * DH
TOK = NBLK * BLK
RING = 4
OUT = 2048
OROWS = TOK // RING
LOCAL = 3
REMOTE = 5
LEVELS = 20
ZERO_LANE = 127


def dot(a, b):
    return jnp.dot(a, b, preferred_element_type=F32)


def dot_t(a, b):
    return lax.dot_general(a, b, (((1,), (1,)), ((), ())), preferred_element_type=F32)


def dot_tl(a, b):
    return lax.dot_general(a, b, (((0,), (0,)), ((), ())), preferred_element_type=F32)


GATHER = lax.GatherDimensionNumbers(
    offset_dims=(),
    collapsed_slice_dims=(1,),
    start_index_map=(1,),
    operand_batching_dims=(0,),
    start_indices_batching_dims=(0,),
)


def pick_lanes(w, at):
    return lax.gather(w, at[..., None], GATHER, (1, 1), mode=lax.GatherScatterMode.PROMISE_IN_BOUNDS)


def beside(*parts):
    return jnp.concatenate(parts, axis=1)


def stacked(*parts):
    return jnp.concatenate(parts, axis=0)


def lanes(w, lane, rows):
    return jnp.broadcast_to(w[:, lane : lane + 1], (rows, DH))


def kernel(
    idx_ref, tab_ref, q_hbm, k_hbm, v_hbm, w_hbm, o_ref,
    qv, kv, vv, wb, wt, pick, leaf, near, tot, tsend, trecv, zr, yr, far, acc, ql_far, nb, rb, own,
    kvsem, qsem, wsem,
    t_s, t_r, z_s, z_r, y_s, y_r, l_s, l_r,
    wx_s, wx_r, wz_s, wz_r, wy_s, wy_r, fz_s, fz_r, fy_s, fy_r, wd_s, wd_r, a_s, a_r,
):
    ctx = lax.axis_index("ctx")
    x = lax.axis_index("mp")
    c = lax.rem(ctx, 2)
    z = lax.rem(ctx // 2, RING)
    y = ctx // (2 * RING)

    def place(yy, zz, cc):
        return (yy * RING + zz) * 2 + cc

    def plus(p, d):
        return lax.rem(p + d, RING)

    partner = {"ctx": place(y, z, 1 - c), "mp": x}

    def zpeer(p):
        return {"ctx": place(y, p, c), "mp": x}

    def ypeer(p):
        return {"ctx": place(p, z, c), "mp": x}

    def xpeer(p):
        return {"ctx": ctx, "mp": p}

    def rcopy(src, dst, s, r, dev):
        return pltpu.make_async_remote_copy(
            src_ref=src, dst_ref=dst, send_sem=s, recv_sem=r, device_id=dev, device_id_type=MESH
        )

    barrier = pltpu.get_barrier_semaphore()
    pl.semaphore_signal(barrier, inc=1, device_id=partner, device_id_type=MESH)
    for d in (1, 2, 3):
        for dev in (zpeer(plus(z, d)), ypeer(plus(y, d)), xpeer(plus(x, d))):
            pl.semaphore_signal(barrier, inc=1, device_id=dev, device_id_type=MESH)

    def rows(n, size=BLK):
        return pl.ds(pl.multiple_of(n * size, size), size)

    def kload(n):
        return pltpu.make_async_copy(k_hbm.at[rows(n)], kv.at[rows(n)], kvsem.at[0, n])

    def vload(n):
        return pltpu.make_async_copy(v_hbm.at[rows(n)], vv.at[rows(n)], kvsem.at[1, n])

    qload = pltpu.make_async_copy(q_hbm, qv, qsem)
    wload = pltpu.make_async_copy(w_hbm, wb.at[x], wsem)
    for n in range(NBLK):
        kload(n).start()
        vload(n).start()
    wload.start()
    qload.start()

    def leaf_body(n, carry):
        kload(n).wait()
        vload(n).wait()

        for h in range(HEADS):
            col = slice(h * DH, (h + 1) * DH)
            leaf[n, h] = dot_tl(kv[rows(n), col], vv[rows(n), col])
        return carry

    lax.fori_loop(0, NBLK, leaf_body, 0)
    for h in range(HEADS):
        total = leaf[0, h]
        for n in range(1, NBLK):
            total = total + leaf[n, h]
        tot[h] = total
        tsend[h] = total.astype(BF)

    pl.semaphore_wait(barrier, 10)
    tcopy = rcopy(tsend, trecv, t_s, t_r, partner)
    tcopy.start()

    def piece_a(quarter, p):
        return wb.at[quarter, rows(p, DH), pl.ds(pl.multiple_of(c * 1024, 1024), 512)]

    def piece_b(quarter, p):
        return wb.at[quarter, rows(p, DH), pl.ds(pl.multiple_of(c * 1024 + 512, 512), 512)]

    def wx_a(quarter, d):
        return rcopy(piece_a(quarter, z), piece_a(quarter, z), wx_s.at[d - 1, 0], wx_r.at[quarter, 0], xpeer(plus(x, d)))

    def wx_b(quarter, d):
        return rcopy(piece_b(quarter, y), piece_b(quarter, y), wx_s.at[d - 1, 1], wx_r.at[quarter, 1], xpeer(plus(x, d)))

    wload.wait()
    for d in (1, 3, 2):
        wx_a(x, d).start()
        wx_b(x, d).start()

    table = jnp.concatenate(
        [tab_ref[:, h, :] for h in range(HEADS)] + [jnp.zeros((16, DH - HEADS * LEVELS), F32)], axis=1
    )
    hi = table.astype(BF)
    rest = table - hi.astype(F32)
    mid = rest.astype(BF)
    low = (rest - mid.astype(F32)).astype(BF)
    table3 = jnp.concatenate([hi, mid, low], axis=0)
    plan = lax.broadcasted_iota(jnp.int32, (16, DH), 0)
    for i in range(TOK // DH):
        hot = (jnp.broadcast_to(idx_ref[i : i + 1, :], (16, DH)) == plan).astype(F32).astype(BF)
        wt[i * DH : (i + 1) * DH, :] = dot_tl(jnp.concatenate([hot, hot, hot], axis=0), table3)
    tt = lax.broadcasted_iota(jnp.int32, (HALF, HALF), 0)
    ss = lax.broadcasted_iota(jnp.int32, (HALF, HALF), 1)
    apart = jnp.bitwise_xor(tt, ss)
    level = jnp.zeros((HALF, HALF), jnp.int32)
    for bit in range(7):
        level = level + (apart >= (1 << bit)).astype(jnp.int32)
    for h in range(HEADS):
        pick[h] = jnp.where(ss <= tt, level + h * LEVELS, ZERO_LANE)

    zero = jnp.zeros((DH, DH), BF)

    for h in range(HEADS):
        l0, l2, l4, l6 = leaf[0, h], leaf[2, h], leaf[4, h], leaf[6, h]
        p0 = l0 + leaf[1, h]
        p4 = l4 + leaf[5, h]
        f0 = p0 + (l2 + leaf[3, h])
        near[h, 0] = zero
        for i, node in enumerate((l0, l2, l4, l6, p0, p4, f0)):
            near[h, 1 + i] = node.astype(BF)
    for p in range(2):
        far[p, 0 : REMOTE * DH, DH:] = jnp.zeros((REMOTE * DH, DH), BF)
        far[p, REMOTE * DH :, :DH] = jnp.zeros((REMOTE * DH, DH), BF)
    qload.wait()

    half0 = c * 2

    def far_at(pair, i, first, count):
        return far.at[pair, pl.ds((i * REMOTE + first) * DH, count * DH), pl.ds(i * DH, DH)]

    def zcopy(src, d, i):
        return rcopy(zr.at[src, i], zr.at[src, i], z_s.at[d - 1, i], z_r.at[src, i], zpeer(plus(z, d)))

    def ycopy(src, d, i):
        return rcopy(yr.at[src, i], yr.at[src, i], y_s.at[d - 1, i], y_r.at[src, i], ypeer(plus(y, d)))

    def lcopy(i):
        mine = far_at(c, i, 1, 4)
        return rcopy(mine, mine, l_s.at[i], l_r.at[i], partner)

    def choose(cond, value):
        return jnp.where(cond, value, jnp.zeros_like(value))

    def exchange_z():
        tcopy.wait_recv()
        for i in range(2):
            zr[z, i] = (tot[half0 + i] + trecv[half0 + i].astype(F32)).astype(BF)
            for d in (2, 1, 3):
                zcopy(z, d, i).start()
        for h in range(HEADS):
            far_at(h // 2, h % 2, 0, 1)[...] = choose(c == 1, trecv[h].astype(F32)).astype(BF)

    def exchange_y(i):
        for d in (1, 2, 3):
            zcopy(plus(z, d), d, i).wait_recv()
        parts = [zr[p, i].astype(F32) for p in range(RING)]
        pair = parts[0] + parts[1]
        yr[y, i] = (pair + (parts[2] + parts[3])).astype(BF)
        for d in (2, 1, 3):

            @pl.when(y + d < RING)
            def _():
                ycopy(y, d, i).start()

        lower = zr[jnp.maximum(z - 1, 0), i].astype(F32)
        far_at(c, i, 1, 1)[...] = choose(lax.rem(z, 2) == 1, lower).astype(BF)
        far_at(c, i, 2, 1)[...] = choose(z >= 2, pair).astype(BF)

    def exchange_end(i):
        for d in (1, 2, 3):

            @pl.when(y >= d)
            def _():
                ycopy(y - d, d, i).wait_recv()

        lower = yr[jnp.maximum(y - 1, 0), i].astype(F32)
        pair = yr[0, i].astype(F32) + yr[1, i].astype(F32)
        far_at(c, i, 3, 1)[...] = choose(lax.rem(y, 2) == 1, lower).astype(BF)
        far_at(c, i, 4, 1)[...] = choose(y >= 2, pair).astype(BF)
        lcopy(i).start()

    exchange_z()

    def attend(n):
        r = rows(n)
        w = wt[r, :]
        w16 = w.astype(BF)
        which = (
            jnp.where(lax.rem(n, 2) == 1, 1 + n // 2, 0),
            jnp.where(lax.rem(n // 2, 2) == 1, jnp.where(n >= 4, 6, 5), 0),
            jnp.where(n >= 4, 7, 0),
        )
        z_lo, z_hi = jnp.zeros((HALF, DH), BF), jnp.zeros((BLK, DH), BF)
        for p in range(2):
            low, high, near_q, values = [], [], [], []
            for h in (2 * p, 2 * p + 1):
                col = slice(h * DH, (h + 1) * DH)
                q, k, v = qv[r, col], kv[r, col], vv[r, col]
                at = pick[h]
                s_lo = dot_t(q[:HALF], k[:HALF])
                s_hi = dot_t(q[HALF:], k)
                low.append((s_lo * pick_lanes(w[:HALF], at)).astype(BF))
                high.append((s_hi[:, :HALF] * lanes(w16[HALF:], h * LEVELS + 8, HALF).astype(F32)).astype(BF))
                high.append((s_hi[:, HALF:] * pick_lanes(w[HALF:], at)).astype(BF))
                for j in range(LOCAL):
                    near_q.append(q * lanes(w16, h * LEVELS + 9 + j, BLK))
                for j in range(REMOTE):
                    ql_far[r, (h * REMOTE + j) * DH : (h * REMOTE + j + 1) * DH] = q * lanes(
                        w16, h * LEVELS + 12 + j, BLK
                    )
                values.append(v)
            va, vb = values
            nodes_a, nodes_b = ([near[h, t] for t in which] for h in (2 * p, 2 * p + 1))
            states = stacked(
                *[beside(t, zero) for t in nodes_a],
                *[beside(zero, t) for t in nodes_b],
            )
            pair = slice(2 * p * DH, 2 * (p + 1) * DH)
            acc[rows(2 * n, HALF), pair] = dot(
                beside(*low, *[t[:HALF] for t in near_q]),
                stacked(beside(va[:HALF], z_lo), beside(z_lo, vb[:HALF]), states),
            )
            acc[rows(2 * n + 1, HALF), pair] = dot(
                beside(*high, *[t[HALF:] for t in near_q]),
                stacked(beside(va, z_hi), beside(z_hi, vb), states),
            )

    order = (2, 1, 3)

    def offset(i):
        return jnp.where(i == 0, order[0], jnp.where(i == 1, order[1], order[2]))

    def attend_sent(i, carry):
        attend(2 * plus(x, offset(lax.rem(i, 3))) + i // 3)
        for at_i, hook in hooks:

            @pl.when(i == at_i)
            def _():
                hook()

        return carry

    def wz(quarter, src, d):
        return rcopy(piece_a(quarter, src), piece_a(quarter, src), wz_s.at[quarter, d - 1], wz_r.at[quarter, src], zpeer(plus(z, d)))

    def wy(quarter, src, d):
        return rcopy(piece_b(quarter, src), piece_b(quarter, src), wy_s.at[quarter, d - 1], wy_r.at[quarter, src], ypeer(plus(y, d)))

    sources = (3, 1, 2)

    def half_a(quarter, p, k):
        return wb.at[quarter, rows(2 * p + k, DH // 2), pl.ds(pl.multiple_of(c * 1024, 1024), 512)]

    def half_b(quarter, p, k):
        return wb.at[quarter, rows(2 * p + k, DH // 2), pl.ds(pl.multiple_of(c * 1024 + 512, 512), 512)]

    def fz(quarter, p, k, d):
        piece = half_a(quarter, p, k)
        return rcopy(piece, piece, fz_s.at[quarter, k], fz_r.at[quarter, k], zpeer(plus(z, d)))

    def fy(quarter, p, k, d):
        piece = half_b(quarter, p, k)
        return rcopy(piece, piece, fy_s.at[quarter, k], fy_r.at[quarter, k], ypeer(plus(y, d)))

    def send_wz(e):
        wx_a(plus(x, e), 1).wait_recv()
        for d in (1, 3):
            wz(plus(x, e), z, d).start()

    def send_wy(e):
        wx_b(plus(x, e), 1).wait_recv()
        for d in (1, 3):
            wy(plus(x, e), y, d).start()

    def forward_z(e):
        quarter = plus(x, e)
        wz(quarter, plus(z, 3), 1).wait_recv()
        fz(quarter, plus(z, 3), 0, 1).start()
        wz(quarter, plus(z, 1), 3).wait_recv()
        fz(quarter, plus(z, 1), 1, 3).start()

    def forward_y(e):
        quarter = plus(x, e)
        wy(quarter, plus(y, 3), 1).wait_recv()
        fy(quarter, plus(y, 3), 0, 1).start()
        wy(quarter, plus(y, 1), 3).wait_recv()
        fy(quarter, plus(y, 1), 1, 3).start()

    def wd(quarter, e, part):
        cols = pl.ds(pl.multiple_of(c * 1024 + part * 512, 512), 512)
        piece = wb.at[quarter, :, cols]
        return rcopy(piece, piece, wd_s.at[e - 1, part], wd_r.at[quarter, part], partner)

    def share_a(e):
        quarter = plus(x, e)
        for k in range(2):
            fz(quarter, plus(z, 2), k, 1 + 2 * k).wait_recv()
        wd(quarter, e, 0).start()

    def share_b(e):
        quarter = plus(x, e)
        for k in range(2):
            fy(quarter, plus(y, 2), k, 1 + 2 * k).wait_recv()
        wd(quarter, e, 1).start()

    hooks = (
        (3, lambda: exchange_y(0)),
        (4, lambda: exchange_y(1)), (5, lambda: (send_wz(3), send_wz(1))),
    )
    lax.fori_loop(0, 6, attend_sent, 0)
    exchange_end(0)
    exchange_end(1)

    def acopy(src, slot, d):
        mine = lax.rem(slot + c, 2)
        block = 2 * plus(src, d)
        if slot < 2:
            cols = pl.ds(pl.multiple_of(mine * 2 * DH, 2 * DH), 2 * DH)
            here = nb.at[rows(block), cols]
            there = rb.at[src, pl.ds(0, BLK), cols]
        else:
            here = nb.at[rows(2 * block + slot, HALF)]
            there = rb.at[src, pl.ds(slot * HALF, HALF)]
        return rcopy(here, there, a_s.at[d - 1, slot], a_r.at[src, slot], xpeer(plus(src, d)))

    def finish(n, pair):
        r = rows(n)
        col = pl.ds(pl.multiple_of(pair * 2 * DH, 2 * DH), 2 * DH)
        wide = pl.ds(pl.multiple_of(pair * 2 * REMOTE * DH, 2 * REMOTE * DH), 2 * REMOTE * DH)
        o = acc[r, col] + dot(ql_far[r, wide], far[pair])
        done = []
        for t in (o[:, :DH], o[:, DH:]):
            ms = jnp.mean(t * t, axis=-1, keepdims=True)
            done.append((t * lax.rsqrt(ms + EPSILON)).astype(BF))
        nb[r, col] = beside(*done)

    def send_slots(i, slots):
        for m, d in enumerate(order):

            @pl.when(i == m)
            def _():
                for slot in slots:
                    acopy(x, slot, d).start()

    def early(slot):
        def body(i, carry):
            finish(2 * plus(x, offset(i)), lax.rem(slot + c, 2))
            send_slots(i, (slot,))
            return carry

        lax.fori_loop(0, 3, body, 0)

    def late(i, carry):
        n = 2 * plus(x, offset(i)) + 1
        finish(n, 0)
        finish(n, 1)
        send_slots(i, (2, 3))
        return carry

    send_wy(3)
    send_wy(1)
    early(0)
    for i in range(2):
        theirs = far_at(1 - c, i, 1, 4)
        rcopy(theirs, theirs, l_s.at[i], l_r.at[i], partner).wait_recv()
    early(1)
    send_wz(2)
    send_wy(2)
    lax.fori_loop(0, 3, late, 0)
    forward_z(3)
    forward_y(3)
    forward_z(1)

    def keep(i, carry):
        attend(2 * x + i)
        finish(2 * x + i, 0)
        finish(2 * x + i, 1)

        @pl.when(i == 0)
        def _():
            forward_y(1)
            forward_z(2)
            share_a(3)
            share_b(3)

        return carry

    lax.fori_loop(0, 2, keep, 0)

    NC = 1024

    def project_own(i, carry):
        cl = rows(i, NC)
        own[:, cl] = dot(nb[rows(x, OROWS), :], wb[x, :, cl])
        return carry

    def project(row, size, es=sources, last=True):
        rws = pl.ds(row, size)

        def body(i, carry):
            cl = rows(i, NC)
            s = dot(rb[plus(x, es[0]), rws, :], wb[plus(x, es[0]), :, cl])
            for e in es[1:]:
                s = s + dot(rb[plus(x, e), rws, :], wb[plus(x, e), :, cl])
            s = s + own[rws, cl]
            if last:
                o_ref[rws, cl] = s.astype(BF)
            else:
                own[rws, cl] = s
            return carry

        lax.fori_loop(0, OUT // NC, body, 0)

    def share_done(e):
        for part in range(2):
            wd(plus(x, e), e, part).wait_recv()

    def arrived(slot, es):
        for e in es:
            acopy(plus(x, e), slot, RING - e).wait_recv()

    forward_y(2)
    share_a(1)
    share_b(1)
    lax.fori_loop(0, OUT // NC, project_own, 0)
    share_a(2)
    share_b(2)
    share_done(3)
    share_done(1)
    share_done(2)
    arrived(0, sources)
    arrived(1, sources)
    project(0, BLK)
    arrived(2, sources)
    project(2 * HALF, HALF)
    arrived(3, (2,))
    project(3 * HALF, HALF, (2,), False)
    arrived(3, (3, 1))
    project(3 * HALF, HALF, (3, 1))

    tcopy.wait_send()
    for i in range(2):
        lcopy(i).wait_send()
    for d in (1, 2, 3):
        for i in range(2):
            zcopy(z, d, i).wait_send()

            @pl.when(y + d < RING)
            def _():
                ycopy(y, d, i).wait_send()

        wx_a(x, d).wait_send()
        wx_b(x, d).wait_send()
        quarter = plus(x, d)
        for k, dd in ((0, 1), (1, 3)):
            wz(quarter, z, dd).wait_send()
            wy(quarter, y, dd).wait_send()
            fz(quarter, plus(z, dd), k, dd).wait_send()
            fy(quarter, plus(y, dd), k, dd).wait_send()
            wd(quarter, d, k).wait_send()
        for slot in range(4):
            acopy(x, slot, d).wait_send()


def body(queries, key_vectors, value_vectors, level_index, level_table, out_weight):
    index = level_index.reshape(TOK // DH, DH)
    anyspec = pl.BlockSpec(memory_space=pl.ANY)
    vspec = pl.BlockSpec(memory_space=pltpu.VMEM)
    dma = pltpu.SemaphoreType.DMA
    scratch = [
        pltpu.VMEM((TOK, COLS), BF),
        pltpu.VMEM((TOK, COLS), BF),
        pltpu.VMEM((TOK, COLS), BF),
        pltpu.VMEM((RING, COLS, OUT), BF),
        pltpu.VMEM((TOK, DH), F32),
        pltpu.VMEM((HEADS, HALF, HALF), jnp.int32),
        pltpu.VMEM((NBLK, HEADS, DH, DH), F32),
        pltpu.VMEM((HEADS, 8, DH, DH), BF),
        pltpu.VMEM((HEADS, DH, DH), F32),
        pltpu.VMEM((HEADS, DH, DH), BF),
        pltpu.VMEM((HEADS, DH, DH), BF),
        pltpu.VMEM((RING, 2, DH, DH), BF),
        pltpu.VMEM((RING, 2, DH, DH), BF),
        pltpu.VMEM((2, 2 * REMOTE * DH, 2 * DH), BF),
        pltpu.VMEM((TOK, COLS), F32),
        pltpu.VMEM((TOK, HEADS * REMOTE * DH), BF),
        pltpu.VMEM((TOK, COLS), BF),
        pltpu.VMEM((RING, OROWS, COLS), BF),
        pltpu.VMEM((OROWS, OUT), F32),
        dma((2, NBLK)), dma, dma,
        dma, dma, dma((3, 2)), dma((RING, 2)), dma((3, 2)), dma((RING, 2)), dma((2,)), dma((2,)),
        dma((3, 2)), dma((RING, 2)), dma((RING, 3)), dma((RING, RING)), dma((RING, 3)), dma((RING, RING)),
        dma((RING, 2)), dma((RING, 2)), dma((RING, 2)), dma((RING, 2)),
        dma((3, 2)), dma((RING, 2)), dma((3, 4)), dma((RING, 4)),
    ]
    return pl.pallas_call(
        kernel,
        out_shape=pltpu.VMEM((OROWS, OUT), BF),
        in_specs=[vspec, vspec, anyspec, anyspec, anyspec, anyspec],
        out_specs=vspec,
        scratch_shapes=scratch,
        compiler_params=pltpu.CompilerParams(
            collective_id=0, has_side_effects=True, vmem_limit_bytes=56 * 1024 * 1024
        ),
    )(index, level_table, queries, key_vectors, value_vectors, out_weight)


def solution(mesh):
    placed = (
        P("ctx", "mp"),
        P("ctx", "mp"),
        P("ctx", "mp"),
        P("ctx"),
        P(None, "mp", None),
        P("mp", None),
    )
    return jax.shard_map(
        body, mesh=mesh, in_specs=placed, out_specs=P(("ctx", "mp"), None), check_vma=False
    )
```
